32 devices in a mesh: clip: 16 (over z, x, core), tm: 2 (over y).
Axes of the slice: x: 2, y: 2, z: 4, core: 2. Of those that a mesh axis runs over, the one named last changes fastest.
Arguments:
- block_input: bfloat16 [16, 4, 32, 4096], P('clip', 'tm'), may hold values from -6 to 6
- input_cache: bfloat16 [16, 2, 32, 4096], P('clip'), may hold values from -6 to 6
- middle_cache: bfloat16 [16, 2, 32, 4096], P('clip'), may hold values from -6 to 6
- first_weight: bfloat16 [3, 3, 3, 64, 64], replicated, may hold values from -0.15625 to 0.15625
- first_bias: float32 [64], replicated, may hold values from -3 to 3
- second_weight: bfloat16 [3, 3, 3, 64, 64], replicated, may hold values from -0.15625 to 0.15625
- cotangent: bfloat16 [16, 4, 32, 4096], P('clip', 'tm'), may hold values from -6 to 6
Outputs:
- input_grad: bfloat16 [16, 4, 32, 4096], P('clip', 'tm')
- input_cache_grad: bfloat16 [16, 2, 32, 4096], P('clip', None, 'tm')
- middle_cache_grad: bfloat16 [16, 2, 32, 4096], P('clip', None, 'tm')
- first_weight_grad: float32 [3, 3, 3, 64, 64], replicated
- second_weight_grad: float32 [3, 3, 3, 64, 64], replicated
The draws below stay inside these ranges and needn't reach their ends.
All inputs are finite; a program needn't handle non-finite values.
Results may differ from the reference program's by a relative error of at most 0.009.
Values may be sent and summed in bfloat16 or wider, within the bound.
A program may use at most 128 MiB of HBM per device.

```python
import jax
import jax.numpy as jnp
from jax import lax

C = 64
H = 32
W = 64
CLIPS = 16
FRAMES = 4


def steps_of(key, extent, pieces, smallest, high):
    factor_of, own = 1.0, jax.random.fold_in(key, 6)
    for position, blocks in pieces:
        heights = jnp.exp(jax.random.uniform(jax.random.fold_in(own, position), (blocks,), jnp.float32, smallest / len(pieces), high / len(pieces)))
        factor_of = factor_of * jnp.repeat(heights, extent[position] // blocks).reshape([-1 if axis == position else 1 for axis in range(len(extent))])
    return factor_of


def normal_values(key, shape, scale, limit, shards=(), kind=jnp.bfloat16):
    result = jax.random.normal(key, shape, jnp.float32) * scale
    if len(shards) > 0:
        result = steps_of(key, shape, shards, -0.22, 0.18) * result
    return jnp.clip(result, min=-limit, max=limit).astype(kind)


def setup_inputs(seed: int = 0) -> dict:
    key_of = jax.random.split(jax.random.key(seed), 8)
    return {
        "block_input": normal_values(key_of[0], (CLIPS, FRAMES, H, W * C), 1.0, 6.0, ((0, 16), (1, 2))),
        "input_cache": normal_values(key_of[1], (CLIPS, 2, H, W * C), 1.0, 6.0, ((0, 16),)),
        "middle_cache": normal_values(key_of[2], (CLIPS, 2, H, W * C), 1.0, 6.0, ((0, 16),)),
        "first_weight": normal_values(key_of[3], (3, 3, 3, C, C), (27 * C) ** -0.5, 0.15625),
        "first_bias": normal_values(key_of[4], (C,), 0.5, 3.0, (), jnp.float32),
        "second_weight": normal_values(key_of[5], (3, 3, 3, C, C), (27 * C) ** -0.5, 0.15625),
        "cotangent": normal_values(key_of[6], (CLIPS, FRAMES, H, W * C), 1.0, 6.0, ((0, 16), (1, 2))),
    }


def conv(source, weight):
    return lax.conv_general_dilated(source.astype(jnp.float32), weight.astype(jnp.float32), (1, 1, 1), ((0, 0), (1, 1), (1, 1)), dimension_numbers=('NDHWC', 'DHWIO', 'NDHWC'), precision=lax.Precision.HIGHEST)

def silu_slope(value):
    logistic = jax.nn.sigmoid(value)
    return logistic * (1.0 + value * (1.0 - logistic))

def reference(block_input, input_cache, middle_cache, first_weight, first_bias, second_weight, cotangent):

    def one_clip(items):
        block, cache_first, cache_second, upstream = items
        shaped = block.reshape(1, FRAMES, H, W, C)
        extended = jnp.concatenate([cache_first.reshape(1, 2, H, W, C), shaped], axis=1)
        activated = jax.nn.silu(extended.astype(jnp.float32)).astype(jnp.bfloat16)
        pre = conv(activated, first_weight) + first_bias
        middle = jax.nn.silu(pre).astype(jnp.bfloat16)
        middle_ext = jnp.concatenate([cache_second.reshape(1, 2, H, W, C), middle], axis=1)
        upstream_f = upstream.reshape(1, FRAMES, H, W, C).astype(jnp.float32)
        unused_out, pull_second = jax.vjp(conv, middle_ext.astype(jnp.float32), second_weight.astype(jnp.float32))
        middle_ext_grad, second_sum = pull_second(upstream_f)
        pre_grad = (middle_ext_grad[:, 2:] * silu_slope(pre)).astype(jnp.bfloat16)
        unused_pre, pull_first = jax.vjp(conv, activated.astype(jnp.float32), first_weight.astype(jnp.float32))
        activated_grad, first_sum = pull_first(pre_grad.astype(jnp.float32))
        extended_grad = activated_grad * silu_slope(extended.astype(jnp.float32))
        input_grad = (upstream_f + extended_grad[:, 2:]).astype(jnp.bfloat16).reshape(FRAMES, H, W * C)
        input_cache_grad = extended_grad[:, :2].astype(jnp.bfloat16).reshape(2, H, W * C)
        middle_cache_grad = middle_ext_grad[:, :2].astype(jnp.bfloat16).reshape(2, H, W * C)
        return (input_grad, input_cache_grad, middle_cache_grad, first_sum, second_sum)
    grads, cache_a, cache_b, first_all, second_all = lax.map(one_clip, (block_input, input_cache, middle_cache, cotangent))
    factor = 1.0 / jnp.sqrt(jnp.float32(CLIPS * FRAMES * H * W))
    first_weight_grad = lax.optimization_barrier(jnp.sum(first_all, axis=0)) * factor
    second_weight_grad = lax.optimization_barrier(jnp.sum(second_all, axis=0)) * factor
    return (grads, cache_a, cache_b, first_weight_grad, second_weight_grad)
```

```python
import functools
import math

import jax
import jax.numpy as jnp
from jax import lax
from jax.experimental import pallas as pl
from jax.experimental.pallas import tpu as pltpu
from jax.sharding import PartitionSpec as P


def group_of(chans, width):
    group = max(1, 128 // chans)
    return group if width % group == 0 else 1


def bands_with_halo(array, axis, halo):
    count = lax.axis_size(axis)
    band = array.shape[2] // count
    padded = jnp.pad(array, ((0, 0), (0, 0), (halo, halo), (0, 0)))
    pieces = [
        lax.slice_in_dim(padded, p * band, p * band + band + 2 * halo, axis=2)
        for p in range(count)
    ]
    return lax.all_to_all(
        jnp.concatenate(pieces, axis=2), axis, split_axis=2, concat_axis=1, tiled=True
    )


def grouped(array, lanes):
    return array.reshape(array.shape[:-1] + (array.shape[-1] // lanes, lanes))


def patches(array, chans):
    zero = ((0, 0), (0, 0), (0, 0))
    before = jnp.pad(array[:, :, :, :-1, -chans:], zero + ((1, 0), (0, 0)))
    after = jnp.pad(array[:, :, :, 1:, :chans], zero + ((0, 1), (0, 0)))
    window = jnp.concatenate([before, array, after], axis=-1)
    rows = array.shape[2] - 2
    return jnp.concatenate([window[:, :, k : k + rows] for k in range(3)], axis=-1)


def matrix_of(weight, group):
    taps = jnp.transpose(weight, (1, 2, 3, 0, 4))
    zero = (0, 0)
    placed = jnp.stack(
        [jnp.pad(taps, (zero, (p, group - 1 - p), zero, zero, zero)) for p in range(group)],
        axis=4,
    )
    return placed.reshape(
        placed.shape[0] * placed.shape[1] * placed.shape[2], -1
    )


def product(source, matrix):
    return lax.dot_general(
        source, matrix, (((source.ndim - 1,), (0,)), ((), ())), preferred_element_type=jnp.float32
    )


def correlate(left, right):
    axes = tuple(range(left.ndim - 1))
    return lax.dot_general(
        left, right, ((axes, axes), ((), ())), preferred_element_type=jnp.float32
    )


def taps_of(block, group, first, second):
    block = block.reshape(3, group + 2, first, 3, group, second)
    total = None
    for p in range(group):
        part = block[:, p : p + 3, :, :, p, :]
        total = part if total is None else total + part
    return total


def silu_slope(value):
    logistic = jax.nn.sigmoid(value)
    return logistic * (1.0 + value * (1.0 - logistic))


def plain_body(
    block_input, input_cache, middle_cache, first_weight, first_bias, second_weight, cotangent
):
    chans = first_weight.shape[3]
    width = block_input.shape[3] // chans
    group = group_of(chans, width)
    lanes = group * chans
    height = block_input.shape[2]
    parts = lax.axis_size("tm")
    band = height // parts
    offset = lax.axis_index("tm") * band
    count = (
        block_input.shape[0] * lax.axis_size("clip") * block_input.shape[1] * parts * height * width
    )
    factor = 1.0 / math.sqrt(count)

    source = bands_with_halo(block_input, "tm", 2)
    upstream = grouped(bands_with_halo(cotangent, "tm", 2), lanes)
    padded_cache = jnp.pad(input_cache, ((0, 0), (0, 0), (2, 2), (0, 0)))
    cache_in = lax.dynamic_slice_in_dim(padded_cache, offset, band + 4, 2)
    cache_mid = grouped(lax.dynamic_slice_in_dim(middle_cache, offset, band, 2), lanes)
    extended = grouped(jnp.concatenate([cache_in, source], axis=1), lanes)
    frames = upstream.shape[1]

    activated = jax.nn.silu(extended.astype(jnp.float32)).astype(jnp.bfloat16)
    activated_patches = patches(activated, chans)
    forward = product(activated_patches, matrix_of(first_weight, group))
    pre = jnp.tile(first_bias, group)
    for kt in range(3):
        pre = pre + forward[:, kt : kt + frames, ..., kt * lanes : (kt + 1) * lanes]
    middle = jax.nn.silu(pre[:, :, 1:-1]).astype(jnp.bfloat16)
    middle_ext = jnp.concatenate([cache_mid, middle], axis=1)

    upstream_patches = patches(upstream, chans)
    middle_taps = jnp.concatenate(
        [middle_ext[:, kt : kt + frames] for kt in range(3)], axis=-1
    )
    second_block = correlate(upstream_patches[:, :, 1:-1], middle_taps)
    second_sum = taps_of(second_block, group, chans, chans) * factor
    second_sum = jnp.transpose(jnp.flip(second_sum, (0, 1)), (3, 0, 1, 4, 2))
    second_sum, upstream_patches = lax.optimization_barrier(
        (second_sum.reshape(-1, lanes), upstream_patches)
    )

    def input_grad_of(source_patches, weight):
        flipped = jnp.transpose(jnp.flip(weight, (1, 2)), (0, 1, 2, 4, 3))
        result = product(source_patches, matrix_of(flipped, group))
        total = None
        for kt in range(3):
            part = jnp.pad(
                result[..., kt * lanes : (kt + 1) * lanes],
                ((0, 0), (kt, 2 - kt), (0, 0), (0, 0), (0, 0)),
            )
            total = part if total is None else total + part
        return total

    middle_ext_grad = input_grad_of(upstream_patches, second_weight)
    row = offset - 1 + lax.broadcasted_iota(jnp.int32, (band + 2, 1, 1), 0)
    inside = (row >= 0) & (row < height)
    pre_grad = jnp.where(inside, middle_ext_grad[:, 2:] * silu_slope(pre), 0.0)
    pre_grad = pre_grad.astype(jnp.bfloat16)

    own_rows = pre_grad[:, :, 1:-1]
    grad_taps = jnp.concatenate(
        [
            jnp.pad(own_rows, ((0, 0), (kt, 2 - kt), (0, 0), (0, 0), (0, 0)))
            for kt in range(3)
        ],
        axis=-1,
    )
    first_block = correlate(activated_patches[:, :, 1:-1], grad_taps)
    first_sum = taps_of(first_block, group, chans, chans) * factor
    first_sum = jnp.transpose(first_sum, (3, 0, 1, 2, 4))
    first_sum, pre_grad = lax.optimization_barrier((first_sum.reshape(-1, lanes), pre_grad))
    first_total, second_total = lax.optimization_barrier(
        lax.psum((first_sum, second_sum), ("clip", "tm"))
    )

    activated_grad = input_grad_of(patches(pre_grad, chans), first_weight)
    own = extended[:, :, 2:-2].astype(jnp.float32)
    extended_grad = activated_grad * silu_slope(own)
    own_grad = upstream[:, :, 2:-2].astype(jnp.float32) + extended_grad[:, 2:]

    def merged(array):
        return array.astype(jnp.bfloat16).reshape(array.shape[:3] + (width * chans,))

    input_grad = lax.all_to_all(merged(own_grad), "tm", split_axis=1, concat_axis=2, tiled=True)
    return (
        input_grad,
        merged(extended_grad[:, :2]),
        merged(middle_ext_grad[:, :2, 1:-1]),
        first_total.reshape(first_weight.shape),
        second_total.reshape(second_weight.shape),
    )


LANES = 128
ROWS = 16
MESH = pl.DeviceIdType.MESH


def plan_of(sizes, block_input, first_weight):
    chans = first_weight.shape[3]
    parts, clips = sizes["tm"], sizes["clip"]
    local = block_input.shape[1]
    height = block_input.shape[2]
    total = block_input.shape[3] // LANES
    own = total // parts
    held = min(own + (1 if parts == 2 else 2), total)
    taps = 9 * chans // ROWS * (6 * chans // LANES)
    rest = clips // 2
    piece = -(-(taps // 2) // rest)
    fits = (
        2 * chans == LANES
        and height % 32 == 0
        and total % parts == 0
        and clips % 2 == 0
        and rest > 1
        and parts > 1
        and local * parts % 2 == 0
    )
    return dict(
        fits=fits,
        chans=chans,
        parts=parts,
        clips=clips,
        local=local,
        frames=local * parts,
        height=height,
        total=total,
        own=own,
        held=held,
        taps=taps,
        rest=rest,
        piece=piece,
        band=height // parts,
        direct=(height // parts) % ROWS == 0,
    )


def kernel(
    plan,
    factor,
    x_ref,
    x_cache_ref,
    mid_cache_ref,
    cot_ref,
    first_ref,
    second_back_ref,
    first_back_ref,
    bias_ref,
    grad_ref,
    x_cache_grad_ref,
    mid_cache_grad_ref,
    first_grad_ref,
    second_grad_ref,
    ext,
    cot,
    mid_cache,
    act_taps,
    cot_taps,
    pre_taps,
    slope,
    middle,
    middle_t,
    pre_t,
    staged,
    grad_out,
    x_cache_out,
    mid_cache_out,
    sums,
    sums_in,
    wire,
    wire_in,
    piece_out,
    piece_in,
    gathered,
    local_sem,
    ex_send,
    ex_recv,
    out_send,
    out_recv,
    core_send,
    core_recv,
    ring_send,
    ring_recv,
    part_send,
    part_recv,
):
    chans, parts, local, frames = plan["chans"], plan["parts"], plan["local"], plan["frames"]
    height, own, held, rest = plan["height"], plan["own"], plan["held"], plan["rest"]
    piece, band, taps = plan["piece"], plan["band"], plan["taps"]
    half_tiles = rest * piece
    width = held * LANES
    me = lax.axis_index("tm")
    clip = lax.axis_index("clip")
    core = lax.rem(clip, 2)
    chip = clip // 2

    def first_group(index):
        return jnp.minimum(jnp.maximum(index * own - 1, 0), plan["total"] - held)

    def partner(step):
        return lax.rem(me + step, parts)

    def chip_partner(step):
        return lax.rem(chip + step, rest) * 2 + core

    begin = first_group(me)
    offset = me * own - begin
    lane0 = pl.multiple_of(begin * LANES, LANES)
    own_lane = pl.multiple_of(me * own * LANES, LANES)

    locals_in = [
        pltpu.make_async_copy(
            x_ref.at[0, :, :, pl.ds(lane0, width)],
            ext.at[pl.ds(2 + me * local, local)],
            local_sem.at[0],
        ),
        pltpu.make_async_copy(
            x_cache_ref.at[0, :, :, pl.ds(lane0, width)], ext.at[pl.ds(0, 2)], local_sem.at[1]
        ),
        pltpu.make_async_copy(
            cot_ref.at[0, :, :, pl.ds(lane0, width)],
            cot.at[pl.ds(me * local, local)],
            local_sem.at[2],
        ),
        pltpu.make_async_copy(
            mid_cache_ref.at[0, :, :, pl.ds(own_lane, own * LANES)], mid_cache, local_sem.at[3]
        ),
    ]
    for copy in locals_in:
        copy.start()

    barrier = pltpu.get_barrier_semaphore()
    for step in range(1, parts):
        pl.semaphore_signal(
            barrier, inc=1, device_id={"tm": partner(step)}, device_id_type=MESH
        )
    pl.semaphore_signal(barrier, inc=1, device_id={"clip": clip + 1 - 2 * core}, device_id_type=MESH)
    for step in range(1, rest):
        pl.semaphore_signal(
            barrier, inc=1, device_id={"clip": chip_partner(step)}, device_id_type=MESH
        )
    pl.semaphore_wait(barrier, parts - 1 + 1 + rest - 1)

    def exchange(index, source, target, base):
        copies = []
        for step in range(1, parts):
            there = partner(step)
            lane = pl.multiple_of(first_group(there) * LANES, LANES)
            copies.append(
                pltpu.make_async_remote_copy(
                    src_ref=source.at[0, :, :, pl.ds(lane, width)],
                    dst_ref=target.at[pl.ds(base + me * local, local)],
                    send_sem=ex_send.at[index, step - 1],
                    recv_sem=ex_recv.at[index, step - 1],
                    device_id={"tm": there},
                    device_id_type=MESH,
                )
            )
        for copy in copies:
            copy.start()
        return copies

    x_copies = exchange(0, x_ref, ext, 2)
    cot_copies = exchange(1, cot_ref, cot, 0)

    lane_of = lax.broadcasted_iota(jnp.int32, ((held + 1) * height, LANES), 1)
    row_of = lax.rem(
        lax.broadcasted_iota(jnp.int32, ((held + 1) * height, LANES), 0), height
    )

    def put_taps(target, frame, value):
        turned = pltpu.roll(value, chans, 1)
        zero = jnp.zeros((height, LANES), jnp.float32)
        moved = jnp.where(
            lane_of < chans,
            jnp.concatenate([zero, turned], axis=0),
            jnp.concatenate([turned, zero], axis=0),
        )
        count = moved.shape[0]
        above = jnp.where(row_of == 0, 0.0, pltpu.roll(moved, 1, 0))
        below = jnp.where(row_of == height - 1, 0.0, pltpu.roll(moved, count - 1, 0))
        for place, part in enumerate((above, moved, below)):
            target[place, frame] = part.astype(jnp.bfloat16).reshape(held + 1, height, LANES)

    def tiles_of(ref, frame):
        return jnp.concatenate(
            [ref[frame, :, l * LANES : (l + 1) * LANES] for l in range(held)], axis=0
        ).astype(jnp.float32)

    def logistic_of(value):
        return 1.0 / (1.0 + jnp.exp(-value))

    def slope_of(value):
        logistic = logistic_of(value)
        return logistic * (1.0 + value * (1.0 - logistic))

    def put_act(frame):
        value = tiles_of(ext, frame)
        put_taps(act_taps, frame, value * logistic_of(value))

    def put_cot(frame):
        put_taps(cot_taps, frame, tiles_of(cot, frame))

    def loop(count, call):
        def step(index, carry):
            call(index)
            return carry

        lax.fori_loop(0, count, step, 0)

    def window(ref, place, frame, start, count):
        left = ref[place, frame, pl.ds(start, count)].reshape(count * height, LANES)
        right = ref[place, frame, pl.ds(start + 1, count)].reshape(count * height, LANES)
        return jnp.concatenate([left, right], axis=1)

    def matrix(ref, early, late, place):
        zero = jnp.zeros((4 * chans, LANES), jnp.bfloat16)
        parts_of = [zero if k is None else ref[k * 3 + place] for k in (early, late)]
        return jnp.concatenate(parts_of, axis=1)

    def pair_product(ref, base, used, start, count, weight_ref, taps_at):
        total = None
        for f in used:
            early, late = taps_at(f)
            for place in range(3):
                part = jnp.dot(
                    window(ref, place, base + f, start, count),
                    matrix(weight_ref, early, late, place),
                    preferred_element_type=jnp.float32,
                )
                total = part if total is None else total + part
        return total

    def inside(k):
        return k if 0 <= k <= 2 else None

    def ahead(f):
        return inside(f), inside(f - 1)

    def behind(f):
        return inside(2 - f), inside(3 - f)

    locals_in[0].wait()
    locals_in[1].wait()
    loop(2, put_act)
    loop(local, lambda f: put_act(2 + me * local + f))
    locals_in[2].wait()
    loop(local, lambda f: put_cot(me * local + f))
    locals_in[3].wait()

    def put_cache(frame):
        joined = jnp.concatenate(
            [mid_cache[frame, :, l * LANES : (l + 1) * LANES] for l in range(own)], axis=0
        )
        middle_t[frame] = jnp.transpose(joined)

    loop(2, put_cache)

    for step, copy in enumerate(x_copies):
        copy.wait_recv()
        there = lax.rem(me + parts - step - 1, parts)
        loop(local, lambda f: put_act(2 + there * local + f))

    bias = bias_ref[...]

    def forward(pair):
        base = 2 * pair
        total = pair_product(act_taps, base, range(4), 0, held, first_ref, ahead)
        for u in range(2):
            pre = total[:, u * LANES : (u + 1) * LANES] + bias
            logistic = logistic_of(pre)
            slope[base + u] = logistic * (1.0 + pre * (1.0 - logistic))
            middle[base + u] = (pre * logistic).astype(jnp.bfloat16).reshape(held, height, LANES)
            mine = middle[base + u, pl.ds(offset, own)].reshape(own * height, LANES)
            middle_t[2 + base + u] = jnp.transpose(mine)

    loop(frames // 2, forward)

    for step, copy in enumerate(cot_copies):
        copy.wait_recv()
        there = lax.rem(me + parts - step - 1, parts)
        loop(local, lambda f: put_cot(there * local + f))

    def lay_out(target, frame, u):
        for l in range(own):
            target[frame, :, l * LANES : (l + 1) * LANES] = staged[u, offset + l].astype(
                target.dtype
            )

    first_pair = pair_product(cot_taps, -2, range(2, 4), 0, held, second_back_ref, behind)
    for u in range(2):
        staged[u] = first_pair[:, u * LANES : (u + 1) * LANES].reshape(held, height, LANES)
    for u in range(2):
        lay_out(mid_cache_out, u, u)

    def send_out(slot, source_of, target_of, local_source):
        copies = []
        for step in range(1, parts):
            there = partner(step)
            copies.append(
                pltpu.make_async_remote_copy(
                    src_ref=source_of(there),
                    dst_ref=target_of,
                    send_sem=out_send.at[slot, step - 1],
                    recv_sem=out_recv.at[slot, step - 1],
                    device_id={"tm": there},
                    device_id_type=MESH,
                )
            )
        copies.append(pltpu.make_async_copy(local_source, target_of, local_sem.at[4 + slot]))
        for copy in copies:
            copy.start()
        return copies

    def band_of(ref, index):
        return ref.at[:, pl.ds(pl.multiple_of(index * band, ROWS), band), :]

    def send_cache(slot, source, target):
        if plan["direct"]:
            return send_out(
                slot,
                lambda there: band_of(source, there),
                target.at[0, :, :, pl.ds(own_lane, own * LANES)],
                band_of(source, me),
            )
        copy = pltpu.make_async_copy(source, target.at[0], local_sem.at[4 + slot])
        copy.start()
        return [copy]

    outgoing = [send_cache(0, mid_cache_out, mid_cache_grad_ref)]

    def put_pre(total, base):
        for u in range(2):
            grad = total[:, u * LANES : (u + 1) * LANES] * slope[base + u]
            put_taps(pre_taps, base + u, grad)
            at = frames + base + u
            middle[at] = grad.astype(jnp.bfloat16).reshape(held, height, LANES)
            mine = middle[at, pl.ds(offset, own)].reshape(own * height, LANES)
            pre_t[base + u] = jnp.transpose(mine)

    def inner_pair(pair):
        base = 2 * pair
        put_pre(
            pair_product(cot_taps, base, range(4), 0, held, second_back_ref, behind), base
        )

    loop(frames // 2 - 1, inner_pair)
    put_pre(
        pair_product(cot_taps, frames - 2, range(2), 0, held, second_back_ref, behind),
        frames - 2,
    )

    half_blocks = taps // 2 // 3
    folded = 3 * chans

    def fold(value):
        low = value[:chans, :folded]
        high = pltpu.roll(value[chans:], 4 * chans - chans, 1)[:, :folded]
        return (low + high) * factor

    def weight_step(index):
        kt, place = index // 3, lax.rem(index, 3)

        def add(frame, carry):
            second, first = carry
            second = second + jnp.dot(
                middle_t[frame + kt],
                window(cot_taps, place, frame, offset, own),
                preferred_element_type=jnp.float32,
            )
            first = first + jnp.dot(
                pre_t[frame],
                window(act_taps, place, frame + kt, offset, own),
                preferred_element_type=jnp.float32,
            )
            return second, first

        carry = (jnp.zeros((LANES, 4 * chans), jnp.float32),) * 2
        for f in range(frames):
            carry = add(f, carry)
        row = jnp.concatenate([fold(carry[0]), fold(carry[1])], axis=1)
        for s in range(chans // ROWS):
            block = index * (chans // ROWS) + s
            place_of = block * 3 + (half_tiles - taps // 2) * (block // half_blocks)
            for c in range(3):
                sums[place_of + c] = row[s * ROWS : (s + 1) * ROWS, c * LANES : (c + 1) * LANES]

    loop(9, weight_step)
    for h in range(2):
        for n in range(taps // 2, half_tiles):
            sums[h * half_tiles + n] = jnp.zeros((ROWS, LANES), jnp.float32)

    mine = core * half_tiles
    other = (1 - core) * half_tiles
    core_peer = {"clip": clip + 1 - 2 * core}
    core_copy = pltpu.make_async_remote_copy(
        src_ref=sums.at[pl.ds(other, half_tiles)],
        dst_ref=sums_in,
        send_sem=core_send.at[0],
        recv_sem=core_recv.at[0],
        device_id=core_peer,
        device_id_type=MESH,
    )
    core_copy.start()

    def put_ext(total, base, cached):
        for u in range(2):
            for l in range(own):
                lane = pl.multiple_of((offset + l) * LANES, LANES)
                value = ext[base + u, :, pl.ds(lane, LANES)].astype(jnp.float32)
                grad = (
                    total[l * height : (l + 1) * height, u * LANES : (u + 1) * LANES]
                    * slope_of(value)
                )
                place = slice(l * LANES, (l + 1) * LANES)
                if cached:
                    x_cache_out[base + u, :, place] = grad.astype(jnp.bfloat16)
                else:
                    given = cot[base + u - 2, :, pl.ds(lane, LANES)].astype(jnp.float32)
                    grad_out[base + u - 2, :, place] = (given + grad).astype(jnp.bfloat16)

    put_ext(
        pair_product(pre_taps, -2, range(2, 4), offset, own, first_back_ref, behind), 0, True
    )
    outgoing.append(send_cache(1, x_cache_out, x_cache_grad_ref))

    core_copy.wait_recv()

    def chip_sum(index):
        total = sums[mine + index] + sums_in[index]
        sums_in[index] = total
        wire[index] = total.astype(jnp.bfloat16)

    loop(half_tiles, chip_sum)
    ring = []
    for step in range(1, rest):
        there = lax.rem(chip + step, rest)
        ring.append(
            pltpu.make_async_remote_copy(
                src_ref=wire.at[pl.ds(there * piece, piece)],
                dst_ref=wire_in.at[step - 1],
                send_sem=ring_send.at[0, step - 1],
                recv_sem=ring_recv.at[0, step - 1],
                device_id={"clip": there * 2 + core},
                device_id_type=MESH,
            )
        )
    for copy in ring:
        copy.start()

    def inner_ext(pair):
        base = 2 * pair
        put_ext(
            pair_product(pre_taps, base - 2, range(4), offset, own, first_back_ref, behind),
            base,
            False,
        )

    for pair in range(1, frames // 2):
        inner_ext(pair)
    put_ext(
        pair_product(pre_taps, frames - 2, range(2), offset, own, first_back_ref, behind),
        frames,
        False,
    )
    outgoing.append(
        send_out(
            2,
            lambda there: grad_out.at[pl.ds(there * local, local)],
            grad_ref.at[0, :, :, pl.ds(own_lane, own * LANES)],
            grad_out.at[pl.ds(me * local, local)],
        )
    )

    for copy in ring:
        copy.wait_recv()

    def slice_sum(index):
        total = sums_in[chip * piece + index]
        for step in range(1, rest):
            total = total + wire_in[step - 1, index].astype(jnp.float32)
        piece_out[index] = total.astype(jnp.bfloat16)

    loop(piece, slice_sum)

    across = []
    for step in range(1, parts):
        across.append(
            pltpu.make_async_remote_copy(
                src_ref=piece_out,
                dst_ref=piece_in.at[me],
                send_sem=part_send.at[step - 1],
                recv_sem=part_recv.at[step - 1],
                device_id={"tm": partner(step)},
                device_id_type=MESH,
            )
        )
    for copy in across:
        copy.start()
    piece_in[me] = piece_out[...]
    for copy in across:
        copy.wait_recv()

    whole = mine + chip * piece

    def part_sum(index):
        total = piece_in[0, index].astype(jnp.float32)
        for p in range(1, parts):
            total = total + piece_in[p, index].astype(jnp.float32)
        gathered[whole + index] = total.astype(jnp.bfloat16)

    loop(piece, part_sum)

    spread = []
    for step in range(1, rest):
        spread.append(
            pltpu.make_async_remote_copy(
                src_ref=gathered.at[pl.ds(whole, piece)],
                dst_ref=gathered.at[pl.ds(whole, piece)],
                send_sem=ring_send.at[1, step - 1],
                recv_sem=ring_recv.at[1, step - 1],
                device_id={"clip": chip_partner(step)},
                device_id_type=MESH,
            )
        )
    for copy in spread:
        copy.start()
    for copy in spread:
        copy.wait_recv()

    last = pltpu.make_async_remote_copy(
        src_ref=gathered.at[pl.ds(mine, half_tiles)],
        dst_ref=gathered.at[pl.ds(mine, half_tiles)],
        send_sem=core_send.at[1],
        recv_sem=core_recv.at[1],
        device_id=core_peer,
        device_id_type=MESH,
    )
    last.start()
    last.wait_recv()

    def unpack(index):
        blocks = []
        for s in range(chans // ROWS):
            block = index * (chans // ROWS) + s
            place_of = block * 3 + (half_tiles - taps // 2) * (block // half_blocks)
            blocks.append(
                jnp.concatenate([gathered[place_of + c] for c in range(3)], axis=1)
            )
        rows = jnp.concatenate(blocks, axis=0).astype(jnp.float32)
        kt, place = index // 3, lax.rem(index, 3)
        for kq in range(3):
            second_grad_ref[(kt * 3 + 2 - place) * 3 + 2 - kq] = rows[
                :, kq * chans : (kq + 1) * chans
            ]
            first_grad_ref[index * 3 + kq] = jnp.transpose(
                rows[:, (3 + kq) * chans : (4 + kq) * chans]
            )

    loop(9, unpack)

    for copies in outgoing:
        copies[-1].wait()
        for copy in copies[:-1]:
            copy.wait()
    for copy in x_copies + cot_copies + [core_copy, last] + ring + across + spread:
        copy.wait_send()


def strips(weight):
    before = jnp.pad(weight, ((0, 0), (0, 0), (0, 1), (0, 0), (0, 0)))
    after = jnp.pad(weight, ((0, 0), (0, 0), (1, 0), (0, 0), (0, 0)))
    joined = jnp.concatenate([before, after], axis=-1)
    return joined.reshape(9, -1, joined.shape[-1])


def turned(weight):
    return jnp.swapaxes(jnp.flip(weight, (1, 2)), 3, 4)


def body(sizes, *arrays):
    (
        block_input,
        input_cache,
        middle_cache,
        first_weight,
        first_bias,
        second_weight,
        cotangent,
    ) = arrays
    plan = plan_of(sizes, block_input, first_weight)
    if not plan["fits"]:
        return plain_body(*arrays)
    chans, parts, local, frames = plan["chans"], plan["parts"], plan["local"], plan["frames"]
    height, own, held, rest = plan["height"], plan["own"], plan["held"], plan["rest"]
    piece, band, total = plan["piece"], plan["band"], plan["total"]
    count = block_input.shape[0] * plan["clips"] * frames * height * total * LANES // chans
    factor = 1.0 / math.sqrt(count)
    wide, mine = held * LANES, own * LANES
    tiles = rest * piece
    bf16, f32 = jnp.bfloat16, jnp.float32
    if plan["direct"]:
        cache_shape = (1, 2, band, total * LANES)
    else:
        cache_shape = (1, 2, height, mine)
    any_spec = pl.BlockSpec(memory_space=pl.ANY)
    vmem_spec = pl.BlockSpec(memory_space=pltpu.VMEM)
    dma = pltpu.SemaphoreType.DMA
    weight_shape = jax.ShapeDtypeStruct((27, chans, chans), f32)
    outs = pl.pallas_call(
        functools.partial(kernel, plan, factor),
        out_shape=(
            jax.ShapeDtypeStruct(block_input.shape, bf16),
            jax.ShapeDtypeStruct(cache_shape, bf16),
            jax.ShapeDtypeStruct(cache_shape, bf16),
            weight_shape,
            weight_shape,
        ),
        in_specs=[any_spec] * 4 + [vmem_spec] * 4,
        out_specs=(any_spec,) * 3 + (vmem_spec,) * 2,
        scratch_shapes=[
            pltpu.VMEM((frames + 2, height, wide), bf16),
            pltpu.VMEM((frames, height, wide), bf16),
            pltpu.VMEM((2, height, mine), bf16),
            pltpu.VMEM((3, frames + 2, held + 1, height, LANES), bf16),
            pltpu.VMEM((3, frames, held + 1, height, LANES), bf16),
            pltpu.VMEM((3, frames, held + 1, height, LANES), bf16),
            pltpu.VMEM((frames, held * height, LANES), f32),
            pltpu.VMEM((2 * frames, held, height, LANES), bf16),
            pltpu.VMEM((frames + 2, LANES, own * height), bf16),
            pltpu.VMEM((frames, LANES, own * height), bf16),
            pltpu.VMEM((2, held, height, LANES), f32),
            pltpu.VMEM((frames, height, mine), bf16),
            pltpu.VMEM((2, height, mine), bf16),
            pltpu.VMEM((2, height, mine), bf16),
            pltpu.VMEM((2 * tiles, ROWS, LANES), f32),
            pltpu.VMEM((tiles, ROWS, LANES), f32),
            pltpu.VMEM((tiles, ROWS, LANES), bf16),
            pltpu.VMEM((rest - 1, piece, ROWS, LANES), bf16),
            pltpu.VMEM((piece, ROWS, LANES), bf16),
            pltpu.VMEM((parts, piece, ROWS, LANES), bf16),
            pltpu.VMEM((2 * tiles, ROWS, LANES), bf16),
            dma((7,)),
            dma((2, parts - 1)),
            dma((2, parts - 1)),
            dma((3, parts - 1)),
            dma((3, parts - 1)),
            dma((2,)),
            dma((2,)),
            dma((2, rest - 1)),
            dma((2, rest - 1)),
            dma((parts - 1,)),
            dma((parts - 1,)),
        ],
        compiler_params=pltpu.CompilerParams(
            collective_id=0, has_side_effects=True, vmem_limit_bytes=60 * 1024 * 1024
        ),
        name="block_backward",
    )(
        block_input,
        input_cache,
        middle_cache,
        cotangent,
        strips(first_weight),
        strips(turned(second_weight)),
        strips(turned(first_weight)),
        jnp.tile(first_bias, LANES // chans).reshape(1, LANES),
    )
    grad, x_cache_grad, mid_cache_grad, first_grad, second_grad = outs
    if not plan["direct"]:
        x_cache_grad, mid_cache_grad = (
            lax.all_to_all(a, "tm", split_axis=2, concat_axis=3, tiled=True)
            for a in (x_cache_grad, mid_cache_grad)
        )
    shape = first_weight.shape
    return (
        grad,
        x_cache_grad,
        mid_cache_grad,
        first_grad.reshape(shape),
        second_grad.reshape(shape),
    )


def solution(mesh):
    return jax.shard_map(
        functools.partial(body, dict(mesh.shape)),
        mesh=mesh,
        in_specs=(
            P("clip", "tm", None, None),
            P("clip", None, None, None),
            P("clip", None, None, None),
            P(),
            P(),
            P(),
            P("clip", "tm", None, None),
        ),
        out_specs=(
            P("clip", "tm", None, None),
            P("clip", None, "tm", None),
            P("clip", None, "tm", None),
            P(),
            P(),
        ),
        check_vma=False,
    )
```

```python
import functools
import math

import jax
import jax.numpy as jnp
from jax import lax
from jax.experimental import pallas as pl
from jax.experimental.pallas import tpu as pltpu
from jax.sharding import PartitionSpec as P


def group_of(chans, width):
    group = max(1, 128 // chans)
    return group if width % group == 0 else 1


def bands_with_halo(array, axis, halo):
    count = lax.axis_size(axis)
    band = array.shape[2] // count
    padded = jnp.pad(array, ((0, 0), (0, 0), (halo, halo), (0, 0)))
    pieces = [
        lax.slice_in_dim(padded, p * band, p * band + band + 2 * halo, axis=2)
        for p in range(count)
    ]
    return lax.all_to_all(
        jnp.concatenate(pieces, axis=2), axis, split_axis=2, concat_axis=1, tiled=True
    )


def grouped(array, lanes):
    return array.reshape(array.shape[:-1] + (array.shape[-1] // lanes, lanes))


def patches(array, chans):
    zero = ((0, 0), (0, 0), (0, 0))
    before = jnp.pad(array[:, :, :, :-1, -chans:], zero + ((1, 0), (0, 0)))
    after = jnp.pad(array[:, :, :, 1:, :chans], zero + ((0, 1), (0, 0)))
    window = jnp.concatenate([before, array, after], axis=-1)
    rows = array.shape[2] - 2
    return jnp.concatenate([window[:, :, k : k + rows] for k in range(3)], axis=-1)


def matrix_of(weight, group):
    taps = jnp.transpose(weight, (1, 2, 3, 0, 4))
    zero = (0, 0)
    placed = jnp.stack(
        [jnp.pad(taps, (zero, (p, group - 1 - p), zero, zero, zero)) for p in range(group)],
        axis=4,
    )
    return placed.reshape(
        placed.shape[0] * placed.shape[1] * placed.shape[2], -1
    )


def product(source, matrix):
    return lax.dot_general(
        source, matrix, (((source.ndim - 1,), (0,)), ((), ())), preferred_element_type=jnp.float32
    )


def correlate(left, right):
    axes = tuple(range(left.ndim - 1))
    return lax.dot_general(
        left, right, ((axes, axes), ((), ())), preferred_element_type=jnp.float32
    )


def taps_of(block, group, first, second):
    block = block.reshape(3, group + 2, first, 3, group, second)
    total = None
    for p in range(group):
        part = block[:, p : p + 3, :, :, p, :]
        total = part if total is None else total + part
    return total


def silu_slope(value):
    logistic = jax.nn.sigmoid(value)
    return logistic * (1.0 + value * (1.0 - logistic))


def plain_body(
    block_input, input_cache, middle_cache, first_weight, first_bias, second_weight, cotangent
):
    chans = first_weight.shape[3]
    width = block_input.shape[3] // chans
    group = group_of(chans, width)
    lanes = group * chans
    height = block_input.shape[2]
    parts = lax.axis_size("tm")
    band = height // parts
    offset = lax.axis_index("tm") * band
    count = (
        block_input.shape[0] * lax.axis_size("clip") * block_input.shape[1] * parts * height * width
    )
    factor = 1.0 / math.sqrt(count)

    source = bands_with_halo(block_input, "tm", 2)
    upstream = grouped(bands_with_halo(cotangent, "tm", 2), lanes)
    padded_cache = jnp.pad(input_cache, ((0, 0), (0, 0), (2, 2), (0, 0)))
    cache_in = lax.dynamic_slice_in_dim(padded_cache, offset, band + 4, 2)
    cache_mid = grouped(lax.dynamic_slice_in_dim(middle_cache, offset, band, 2), lanes)
    extended = grouped(jnp.concatenate([cache_in, source], axis=1), lanes)
    frames = upstream.shape[1]

    activated = jax.nn.silu(extended.astype(jnp.float32)).astype(jnp.bfloat16)
    activated_patches = patches(activated, chans)
    forward = product(activated_patches, matrix_of(first_weight, group))
    pre = jnp.tile(first_bias, group)
    for kt in range(3):
        pre = pre + forward[:, kt : kt + frames, ..., kt * lanes : (kt + 1) * lanes]
    middle = jax.nn.silu(pre[:, :, 1:-1]).astype(jnp.bfloat16)
    middle_ext = jnp.concatenate([cache_mid, middle], axis=1)

    upstream_patches = patches(upstream, chans)
    middle_taps = jnp.concatenate(
        [middle_ext[:, kt : kt + frames] for kt in range(3)], axis=-1
    )
    second_block = correlate(upstream_patches[:, :, 1:-1], middle_taps)
    second_sum = taps_of(second_block, group, chans, chans) * factor
    second_sum = jnp.transpose(jnp.flip(second_sum, (0, 1)), (3, 0, 1, 4, 2))
    second_sum, upstream_patches = lax.optimization_barrier(
        (second_sum.reshape(-1, lanes), upstream_patches)
    )

    def input_grad_of(source_patches, weight):
        flipped = jnp.transpose(jnp.flip(weight, (1, 2)), (0, 1, 2, 4, 3))
        result = product(source_patches, matrix_of(flipped, group))
        total = None
        for kt in range(3):
            part = jnp.pad(
                result[..., kt * lanes : (kt + 1) * lanes],
                ((0, 0), (kt, 2 - kt), (0, 0), (0, 0), (0, 0)),
            )
            total = part if total is None else total + part
        return total

    middle_ext_grad = input_grad_of(upstream_patches, second_weight)
    row = offset - 1 + lax.broadcasted_iota(jnp.int32, (band + 2, 1, 1), 0)
    inside = (row >= 0) & (row < height)
    pre_grad = jnp.where(inside, middle_ext_grad[:, 2:] * silu_slope(pre), 0.0)
    pre_grad = pre_grad.astype(jnp.bfloat16)

    own_rows = pre_grad[:, :, 1:-1]
    grad_taps = jnp.concatenate(
        [
            jnp.pad(own_rows, ((0, 0), (kt, 2 - kt), (0, 0), (0, 0), (0, 0)))
            for kt in range(3)
        ],
        axis=-1,
    )
    first_block = correlate(activated_patches[:, :, 1:-1], grad_taps)
    first_sum = taps_of(first_block, group, chans, chans) * factor
    first_sum = jnp.transpose(first_sum, (3, 0, 1, 2, 4))
    first_sum, pre_grad = lax.optimization_barrier((first_sum.reshape(-1, lanes), pre_grad))
    first_total, second_total = lax.optimization_barrier(
        lax.psum((first_sum, second_sum), ("clip", "tm"))
    )

    activated_grad = input_grad_of(patches(pre_grad, chans), first_weight)
    own = extended[:, :, 2:-2].astype(jnp.float32)
    extended_grad = activated_grad * silu_slope(own)
    own_grad = upstream[:, :, 2:-2].astype(jnp.float32) + extended_grad[:, 2:]

    def merged(array):
        return array.astype(jnp.bfloat16).reshape(array.shape[:3] + (width * chans,))

    input_grad = lax.all_to_all(merged(own_grad), "tm", split_axis=1, concat_axis=2, tiled=True)
    return (
        input_grad,
        merged(extended_grad[:, :2]),
        merged(middle_ext_grad[:, :2, 1:-1]),
        first_total.reshape(first_weight.shape),
        second_total.reshape(second_weight.shape),
    )


LANES = 128
ROWS = 16
MESH = pl.DeviceIdType.MESH


def plan_of(sizes, block_input, first_weight):
    chans = first_weight.shape[3]
    parts, clips = sizes["tm"], sizes["clip"]
    local = block_input.shape[1]
    height = block_input.shape[2]
    total = block_input.shape[3] // LANES
    own = total // parts
    held = min(own + (1 if parts == 2 else 2), total)
    taps = 27 * chans // 2 // ROWS
    rest = clips // 2
    merged = rest * parts <= 16
    group = rest * parts if merged else rest
    piece = -(-(taps // 2) // group)
    fits = (
        2 * chans == LANES
        and height % 32 == 0
        and total % parts == 0
        and clips % 2 == 0
        and rest > 1
        and parts > 1
        and local % 2 == 0
        and taps % 2 == 0
    )
    return dict(
        fits=fits,
        chans=chans,
        parts=parts,
        clips=clips,
        local=local,
        frames=local * parts,
        height=height,
        total=total,
        own=own,
        held=held,
        taps=taps,
        rest=rest,
        merged=merged,
        group=group,
        piece=piece,
        band=height // parts,
        direct=(height // parts) % ROWS == 0,
    )


def kernel(
    plan,
    factor,
    x_ref,
    x_cache_ref,
    mid_cache_ref,
    cot_ref,
    first_weight_ref,
    second_weight_ref,
    bias_ref,
    grad_ref,
    x_cache_grad_ref,
    mid_cache_grad_ref,
    gathered_ref,
    ext,
    cot,
    mid_cache,
    act_taps,
    cot_taps,
    pre_taps,
    slope,
    middle,
    middle_t,
    pre_t,
    staged,
    grad_out,
    x_cache_out,
    mid_cache_out,
    sums,
    sums_in,
    wire_own,
    wire,
    wire_in,
    piece_out,
    piece_in,
    gathered,
    first_ref,
    second_back_ref,
    first_back_ref,
    second_acc,
    local_sem,
    ex_send,
    ex_recv,
    out_send,
    out_recv,
    core_send,
    core_recv,
    ring_send,
    ring_recv,
    part_send,
    part_recv,
):
    chans, parts, local, frames = plan["chans"], plan["parts"], plan["local"], plan["frames"]
    height, own, held, rest = plan["height"], plan["own"], plan["held"], plan["rest"]
    group, merged = plan["group"], plan["merged"]
    piece, band, taps = plan["piece"], plan["band"], plan["taps"]
    half_tiles = group * piece
    filled = taps // 2
    width = held * LANES
    me = lax.axis_index("tm")
    clip = lax.axis_index("clip")
    core = lax.rem(clip, 2)
    chip = clip // 2

    def first_group(index):
        return jnp.minimum(jnp.maximum(index * own - 1, 0), plan["total"] - held)

    def partner(step):
        return lax.rem(me + step, parts)

    rank = me * rest + chip if merged else chip

    def peer(step):
        there = lax.rem(rank + step, group)
        if merged:
            return there, {"clip": lax.rem(there, rest) * 2 + core, "tm": there // rest}
        return there, {"clip": there * 2 + core}

    core_peer = {"clip": clip + 1 - 2 * core}

    begin = first_group(me)
    offset = me * own - begin
    lane0 = pl.multiple_of(begin * LANES, LANES)
    own_lane = pl.multiple_of(me * own * LANES, LANES)

    locals_in = [
        pltpu.make_async_copy(
            x_ref.at[0, :, :, pl.ds(lane0, width)],
            ext.at[pl.ds(2 + me * local, local)],
            local_sem.at[0],
        ),
        pltpu.make_async_copy(
            x_cache_ref.at[0, :, :, pl.ds(lane0, width)], ext.at[pl.ds(0, 2)], local_sem.at[1]
        ),
        pltpu.make_async_copy(
            cot_ref.at[0, :, :, pl.ds(lane0, width)],
            cot.at[pl.ds(me * local, local)],
            local_sem.at[2],
        ),
        pltpu.make_async_copy(
            mid_cache_ref.at[0, :, :, pl.ds(own_lane, own * LANES)], mid_cache, local_sem.at[3]
        ),
    ]
    for copy in locals_in:
        copy.start()

    barrier = pltpu.get_barrier_semaphore()
    greeted = [core_peer] + [peer(step)[1] for step in range(1, group)]
    if not merged:
        greeted += [{"tm": partner(step)} for step in range(1, parts)]
    for there in greeted:
        pl.semaphore_signal(barrier, inc=1, device_id=there, device_id_type=MESH)
    pl.semaphore_wait(barrier, len(greeted))

    def exchange(index, source, target, base):
        copies = []
        for step in range(1, parts):
            there = partner(step)
            lane = pl.multiple_of(first_group(there) * LANES, LANES)
            copies.append(
                pltpu.make_async_remote_copy(
                    src_ref=source.at[0, :, :, pl.ds(lane, width)],
                    dst_ref=target.at[pl.ds(base + me * local, local)],
                    send_sem=ex_send.at[index, step - 1],
                    recv_sem=ex_recv.at[index, step - 1],
                    device_id={"tm": there},
                    device_id_type=MESH,
                )
            )
        for copy in copies:
            copy.start()
        return copies

    x_copies = exchange(0, x_ref, ext, 2)
    cot_copies = exchange(1, cot_ref, cot, 0)

    lane_of = lax.broadcasted_iota(jnp.int32, ((held + 1) * height, LANES), 1)
    row_of = lax.rem(
        lax.broadcasted_iota(jnp.int32, ((held + 1) * height, LANES), 0), height
    )

    def put_taps(target, frame, value):
        turned = pltpu.roll(value, chans, 1)
        zero = jnp.zeros((height, LANES), jnp.float32)
        moved = jnp.where(
            lane_of < chans,
            jnp.concatenate([zero, turned], axis=0),
            jnp.concatenate([turned, zero], axis=0),
        )
        count = moved.shape[0]
        above = jnp.where(row_of == 0, 0.0, pltpu.roll(moved, 1, 0))
        below = jnp.where(row_of == height - 1, 0.0, pltpu.roll(moved, count - 1, 0))
        for place, part in enumerate((above, moved, below)):
            target[place, frame] = part.astype(jnp.bfloat16).reshape(held + 1, height, LANES)

    def tiles_of(ref, frame):
        return jnp.concatenate(
            [ref[frame, :, l * LANES : (l + 1) * LANES] for l in range(held)], axis=0
        ).astype(jnp.float32)

    def logistic_of(value):
        return 1.0 / (1.0 + jnp.exp(-value))

    def slope_of(value):
        logistic = logistic_of(value)
        return logistic * (1.0 + value * (1.0 - logistic))

    def put_act(frame):
        value = tiles_of(ext, frame)
        put_taps(act_taps, frame, value * logistic_of(value))

    def put_cot(frame):
        put_taps(cot_taps, frame, tiles_of(cot, frame))

    def loop(count, call):
        def step(index, carry):
            call(index)
            return carry

        lax.fori_loop(0, count, step, 0)

    def window(ref, place, frame, start, count):
        left = ref[place, frame, pl.ds(start, count)].reshape(count * height, LANES)
        right = ref[place, frame, pl.ds(start + 1, count)].reshape(count * height, LANES)
        return jnp.concatenate([left, right], axis=1)

    def matrix(ref, early, late, place):
        zero = jnp.zeros((4 * chans, LANES), jnp.bfloat16)
        parts_of = [zero if k is None else ref[k * 3 + place] for k in (early, late)]
        return jnp.concatenate(parts_of, axis=1)

    def pair_product(ref, base, used, start, count, weight_ref, taps_at):
        total = None
        for f in used:
            early, late = taps_at(f)
            for place in range(3):
                part = jnp.dot(
                    window(ref, place, base + f, start, count),
                    matrix(weight_ref, early, late, place),
                    preferred_element_type=jnp.float32,
                )
                total = part if total is None else total + part
        return total

    def inside(k):
        return k if 0 <= k <= 2 else None

    def ahead(f):
        return inside(f), inside(f - 1)

    def behind(f):
        return inside(2 - f), inside(3 - f)

    locals_in[0].wait()
    locals_in[1].wait()
    loop(2, put_act)
    loop(local, lambda f: put_act(2 + me * local + f))
    locals_in[2].wait()
    loop(local, lambda f: put_cot(me * local + f))
    locals_in[3].wait()

    def put_cache(frame):
        joined = jnp.concatenate(
            [mid_cache[frame, :, l * LANES : (l + 1) * LANES] for l in range(own)], axis=0
        )
        middle_t[frame] = jnp.transpose(joined)

    loop(2, put_cache)

    def strip(target, at, pieces):
        none = jnp.zeros((chans, chans), jnp.bfloat16)
        for place in range(4):
            left = pieces[place] if place < 3 else none
            right = pieces[place - 1] if place > 0 else none
            target[at, place * chans : (place + 1) * chans] = jnp.concatenate(
                [left, right], axis=1
            )

    def put_strips(index):
        strip(first_ref, index, [first_weight_ref[index * 3 + kq] for kq in range(3)])
        flipped = (index // 3 * 3 + 2 - lax.rem(index, 3)) * 3 + 2
        for target, source in (
            (second_back_ref, second_weight_ref),
            (first_back_ref, first_weight_ref),
        ):
            strip(target, index, [jnp.transpose(source[flipped - kq]) for kq in range(3)])

    loop(9, put_strips)

    for step, copy in enumerate(x_copies):
        copy.wait_recv()
        there = lax.rem(me + parts - step - 1, parts)
        loop(local, lambda f: put_act(2 + there * local + f))

    bias = bias_ref[...].reshape(1, chans)
    bias = jnp.concatenate([bias] * (LANES // chans), axis=1)

    def forward(pair):
        base = 2 * pair
        total = pair_product(act_taps, base, range(4), 0, held, first_ref, ahead)
        for u in range(2):
            pre = total[:, u * LANES : (u + 1) * LANES] + bias
            logistic = logistic_of(pre)
            slope[base + u] = logistic * (1.0 + pre * (1.0 - logistic))
            middle[base + u] = (pre * logistic).astype(jnp.bfloat16).reshape(held, height, LANES)
            mine = middle[base + u, pl.ds(offset, own)].reshape(own * height, LANES)
            middle_t[2 + base + u] = jnp.transpose(mine)

    loop(frames // 2, forward)

    def second_part(block, fresh):
        def at(place):
            total = None
            for f in range(local):
                frame = block * local + f
                left = middle_t[pl.ds(frame, 3)].reshape(3 * LANES, own * height)
                part = jnp.dot(
                    left,
                    window(cot_taps, place, frame, offset, own),
                    preferred_element_type=jnp.float32,
                )
                total = part if total is None else total + part
            second_acc[place] = total if fresh else second_acc[place] + total

        loop(3, at)

    second_part(me, True)
    for step, copy in enumerate(cot_copies):
        copy.wait_recv()
        there = lax.rem(me + parts - step - 1, parts)
        loop(local, lambda f: put_cot(there * local + f))
        second_part(there, False)

    half_lane = lax.broadcasted_iota(jnp.int32, (chans // 2, LANES), 1)

    def put_sum(which, index, value):
        value = value[:chans] + pltpu.roll(value[chans:], 3 * chans, 1)
        value = value * factor
        low, high = value[:, :LANES], value[:, LANES:]
        half = chans // 2
        tail = jnp.where(half_lane < chans, high[:half], pltpu.roll(high[half:], chans, 1))
        rows = jnp.concatenate([low, tail], axis=0)
        for n in range(3 * chans // 2 // ROWS):
            tile = index * (3 * chans // 2 // ROWS) + n
            tile = tile + (half_tiles - filled) * (tile // filled)
            sums[which, tile] = rows[n * ROWS : (n + 1) * ROWS]

    def put_second(place):
        value = second_acc[place]
        for kt in range(3):
            put_sum(0, kt * 3 + place, value[kt * LANES : (kt + 1) * LANES])

    mine = core * half_tiles
    other = (1 - core) * half_tiles
    whole = mine + rank * piece
    core_copies, ring, across, spread, last = [], [], [], [], []

    def swap_cores(which):
        for h in range(2):
            for n in range(filled, half_tiles):
                sums[which, h * half_tiles + n] = jnp.zeros((ROWS, LANES), jnp.float32)
        core_copies.append(
            pltpu.make_async_remote_copy(
                src_ref=sums.at[which, pl.ds(other, half_tiles)],
                dst_ref=sums_in.at[which],
                send_sem=core_send.at[0, which],
                recv_sem=core_recv.at[0, which],
                device_id=core_peer,
                device_id_type=MESH,
            )
        )
        core_copies[-1].start()

    def scatter(which):
        core_copies[which].wait_recv()

        def chip_sum(index):
            total = sums[which, mine + index] + sums_in[which, index]
            wire_own[which, index] = total
            wire[which, index] = total.astype(jnp.bfloat16)

        loop(half_tiles, chip_sum)
        copies = []
        for step in range(1, group):
            there, device = peer(step)
            copies.append(
                pltpu.make_async_remote_copy(
                    src_ref=wire.at[which, pl.ds(there * piece, piece)],
                    dst_ref=wire_in.at[which, step - 1],
                    send_sem=ring_send.at[0, which, step - 1],
                    recv_sem=ring_recv.at[0, which, step - 1],
                    device_id=device,
                    device_id_type=MESH,
                )
            )
        for copy in copies:
            copy.start()
        ring.append(copies)

    def gather(which):
        for copy in ring[which]:
            copy.wait_recv()

        def slice_sum(index):
            total = wire_own[which, rank * piece + index]
            for step in range(1, group):
                total = total + wire_in[which, step - 1, index].astype(jnp.float32)
            piece_out[which, index] = total.astype(jnp.bfloat16)

        loop(piece, slice_sum)
        if merged:
            gathered[which, pl.ds(whole, piece)] = piece_out[which]
        else:
            copies = []
            for step in range(1, parts):
                copies.append(
                    pltpu.make_async_remote_copy(
                        src_ref=piece_out.at[which],
                        dst_ref=piece_in.at[which, me],
                        send_sem=part_send.at[which, step - 1],
                        recv_sem=part_recv.at[which, step - 1],
                        device_id={"tm": partner(step)},
                        device_id_type=MESH,
                    )
                )
            for copy in copies:
                copy.start()
            across.extend(copies)
            piece_in[which, me] = piece_out[which]
            for copy in copies:
                copy.wait_recv()

            def part_sum(index):
                total = piece_in[which, 0, index].astype(jnp.float32)
                for p in range(1, parts):
                    total = total + piece_in[which, p, index].astype(jnp.float32)
                gathered[which, whole + index] = total.astype(jnp.bfloat16)

            loop(piece, part_sum)
        copies = []
        for step in range(1, group):
            copies.append(
                pltpu.make_async_remote_copy(
                    src_ref=gathered.at[which, pl.ds(whole, piece)],
                    dst_ref=gathered.at[which, pl.ds(whole, piece)],
                    send_sem=ring_send.at[1, which, step - 1],
                    recv_sem=ring_recv.at[1, which, step - 1],
                    device_id=peer(step)[1],
                    device_id_type=MESH,
                )
            )
        for copy in copies:
            copy.start()
        spread.append(copies)

    def share(which):
        for copy in spread[which]:
            copy.wait_recv()
        last.append(
            pltpu.make_async_remote_copy(
                src_ref=gathered.at[which, pl.ds(mine, half_tiles)],
                dst_ref=gathered.at[which, pl.ds(mine, half_tiles)],
                send_sem=core_send.at[1, which],
                recv_sem=core_recv.at[1, which],
                device_id=core_peer,
                device_id_type=MESH,
            )
        )
        last[-1].start()

    loop(3, put_second)
    swap_cores(0)

    def lay_out(target, frame, u):
        for l in range(own):
            target[frame, :, l * LANES : (l + 1) * LANES] = staged[u, offset + l].astype(
                target.dtype
            )

    first_pair = pair_product(cot_taps, -2, range(2, 4), 0, held, second_back_ref, behind)
    for u in range(2):
        staged[u] = first_pair[:, u * LANES : (u + 1) * LANES].reshape(held, height, LANES)
    for u in range(2):
        lay_out(mid_cache_out, u, u)

    def send_out(slot, source_of, target_of, local_source):
        copies = []
        for step in range(1, parts):
            there = partner(step)
            copies.append(
                pltpu.make_async_remote_copy(
                    src_ref=source_of(there),
                    dst_ref=target_of,
                    send_sem=out_send.at[slot, step - 1],
                    recv_sem=out_recv.at[slot, step - 1],
                    device_id={"tm": there},
                    device_id_type=MESH,
                )
            )
        copies.append(pltpu.make_async_copy(local_source, target_of, local_sem.at[4 + slot]))
        for copy in copies:
            copy.start()
        return copies

    def band_of(ref, index):
        return ref.at[:, pl.ds(pl.multiple_of(index * band, ROWS), band), :]

    def send_cache(slot, source, target):
        if plan["direct"]:
            return send_out(
                slot,
                lambda there: band_of(source, there),
                target.at[0, :, :, pl.ds(own_lane, own * LANES)],
                band_of(source, me),
            )
        copy = pltpu.make_async_copy(source, target.at[0], local_sem.at[4 + slot])
        copy.start()
        return [copy]

    scatter(0)
    outgoing = [send_cache(0, mid_cache_out, mid_cache_grad_ref)]

    def put_pre(total, base):
        for u in range(2):
            grad = total[:, u * LANES : (u + 1) * LANES] * slope[base + u]
            put_taps(pre_taps, base + u, grad)
            at = frames + base + u
            middle[at] = grad.astype(jnp.bfloat16).reshape(held, height, LANES)
            mine = middle[at, pl.ds(offset, own)].reshape(own * height, LANES)
            pre_t[base + u] = jnp.transpose(mine)

    def inner_pair(pair):
        base = 2 * pair
        put_pre(
            pair_product(cot_taps, base, range(4), 0, held, second_back_ref, behind), base
        )

    loop(frames // 2 - 1, inner_pair)
    put_pre(
        pair_product(cot_taps, frames - 2, range(2), 0, held, second_back_ref, behind),
        frames - 2,
    )

    def first_at(place):
        totals = [None] * 3
        for m in range(frames + 2):
            t0, t1 = max(0, m - 2), min(frames - 1, m)
            count = t1 - t0 + 1
            part = jnp.dot(
                pre_t[t0 : t1 + 1].reshape(count * LANES, own * height),
                window(act_taps, place, m, offset, own),
                preferred_element_type=jnp.float32,
            )
            for t in range(t0, t1 + 1):
                piece_of = part[(t - t0) * LANES : (t - t0 + 1) * LANES]
                kt = m - t
                totals[kt] = piece_of if totals[kt] is None else totals[kt] + piece_of
        for kt in range(3):
            put_sum(1, kt * 3 + place, totals[kt])

    loop(3, first_at)
    swap_cores(1)

    def put_ext(total, base, cached):
        for u in range(2):
            for l in range(own):
                lane = pl.multiple_of((offset + l) * LANES, LANES)
                value = ext[base + u, :, pl.ds(lane, LANES)].astype(jnp.float32)
                grad = (
                    total[l * height : (l + 1) * height, u * LANES : (u + 1) * LANES]
                    * slope_of(value)
                )
                place = slice(l * LANES, (l + 1) * LANES)
                if cached:
                    x_cache_out[base + u, :, place] = grad.astype(jnp.bfloat16)
                else:
                    given = cot[base + u - 2, :, pl.ds(lane, LANES)].astype(jnp.float32)
                    grad_out[base + u - 2, :, place] = (given + grad).astype(jnp.bfloat16)

    put_ext(
        pair_product(pre_taps, -2, range(2, 4), offset, own, first_back_ref, behind), 0, True
    )
    scatter(1)
    outgoing.append(send_cache(1, x_cache_out, x_cache_grad_ref))

    def inner_ext(pair):
        base = 2 * pair
        put_ext(
            pair_product(pre_taps, base - 2, range(4), offset, own, first_back_ref, behind),
            base,
            False,
        )

    for pair in range(1, frames // 2):
        inner_ext(pair)
    put_ext(
        pair_product(pre_taps, frames - 2, range(2), offset, own, first_back_ref, behind),
        frames,
        False,
    )
    outgoing.append(
        send_out(
            2,
            lambda there: grad_out.at[pl.ds(there * local, local)],
            grad_ref.at[0, :, :, pl.ds(own_lane, own * LANES)],
            grad_out.at[pl.ds(me * local, local)],
        )
    )

    gather(0)
    gather(1)
    share(0)
    share(1)
    done = []
    for which in range(2):
        last[which].wait_recv()
        done.append(
            pltpu.make_async_copy(
                gathered.at[which], gathered_ref.at[which], local_sem.at[7 + which]
            )
        )
        done[-1].start()
    for copy in done:
        copy.wait()

    for copies in outgoing:
        copies[-1].wait()
        for copy in copies[:-1]:
            copy.wait()
    for copy in x_copies + cot_copies + core_copies + across + last:
        copy.wait_send()
    for copies in ring + spread:
        for copy in copies:
            copy.wait_send()


def finish(plan, *refs):
    sources, gathered, targets = refs[:3], refs[3], refs[4:7]
    first_grad_ref, second_grad_ref = refs[7:9]
    buffers, sems = refs[9:12], refs[12]
    chans, taps = plan["chans"], plan["taps"]
    filled, half_tiles = taps // 2, plan["group"] * plan["piece"]
    arriving = [
        pltpu.make_async_copy(source, buffer, sems.at[0, n])
        for n, (source, buffer) in enumerate(zip(sources, buffers))
    ]
    leaving = [
        pltpu.make_async_copy(buffer, target, sems.at[1, n])
        for n, (buffer, target) in enumerate(zip(buffers, targets))
    ]
    for copy in arriving:
        copy.start()

    def rows_of(which, index):
        tiles = []
        for n in range(3 * chans // 2 // ROWS):
            tile = index * (3 * chans // 2 // ROWS) + n
            tiles.append(gathered[which, tile + (half_tiles - filled) * (tile // filled)])
        rows = jnp.concatenate(tiles, axis=0).astype(jnp.float32)
        tail = jnp.concatenate([rows[chans:, :chans], rows[chans:, chans:]], axis=0)
        return rows[:chans, :chans], rows[:chans, chans:], tail

    def step(index, carry):
        kt, place = index // 3, lax.rem(index, 3)
        for kq, value in enumerate(rows_of(0, index)):
            second_grad_ref[(kt * 3 + 2 - place) * 3 + 2 - kq] = value
        for kq, value in enumerate(rows_of(1, index)):
            first_grad_ref[index * 3 + kq] = jnp.transpose(value)
        return carry

    for here, there in zip(arriving, leaving):
        here.wait()
        there.start()
    lax.fori_loop(0, 9, step, 0)
    for copy in leaving:
        copy.wait()


def body(sizes, *arrays):
    (
        block_input,
        input_cache,
        middle_cache,
        first_weight,
        first_bias,
        second_weight,
        cotangent,
    ) = arrays
    plan = plan_of(sizes, block_input, first_weight)
    if not plan["fits"]:
        return plain_body(*arrays)
    chans, parts, local, frames = plan["chans"], plan["parts"], plan["local"], plan["frames"]
    height, own, held, rest = plan["height"], plan["own"], plan["held"], plan["rest"]
    piece, band, total = plan["piece"], plan["band"], plan["total"]
    count = block_input.shape[0] * plan["clips"] * frames * height * total * LANES // chans
    factor = 1.0 / math.sqrt(count)
    wide, mine = held * LANES, own * LANES
    group = plan["group"]
    tiles = group * piece
    bf16, f32 = jnp.bfloat16, jnp.float32
    if plan["direct"]:
        cache_shape = (1, 2, band, total * LANES)
    else:
        cache_shape = (1, 2, height, mine)
    any_spec = pl.BlockSpec(memory_space=pl.ANY)
    vmem_spec = pl.BlockSpec(memory_space=pltpu.VMEM)
    dma = pltpu.SemaphoreType.DMA
    weight_shape = jax.ShapeDtypeStruct((27, chans, chans), f32)
    outs = pl.pallas_call(
        functools.partial(kernel, plan, factor),
        out_shape=(
            jax.ShapeDtypeStruct(block_input.shape, bf16),
            jax.ShapeDtypeStruct(cache_shape, bf16),
            jax.ShapeDtypeStruct(cache_shape, bf16),
            jax.ShapeDtypeStruct((2, 2 * tiles, ROWS, LANES), bf16),
        ),
        in_specs=[any_spec] * 4 + [vmem_spec] * 3,
        out_specs=(any_spec,) * 4,
        scratch_shapes=[
            pltpu.VMEM((frames + 2, height, wide), bf16),
            pltpu.VMEM((frames, height, wide), bf16),
            pltpu.VMEM((2, height, mine), bf16),
            pltpu.VMEM((3, frames + 2, held + 1, height, LANES), bf16),
            pltpu.VMEM((3, frames, held + 1, height, LANES), bf16),
            pltpu.VMEM((3, frames, held + 1, height, LANES), bf16),
            pltpu.VMEM((frames, held * height, LANES), f32),
            pltpu.VMEM((2 * frames, held, height, LANES), bf16),
            pltpu.VMEM((frames + 2, LANES, own * height), bf16),
            pltpu.VMEM((frames, LANES, own * height), bf16),
            pltpu.VMEM((2, held, height, LANES), f32),
            pltpu.VMEM((frames, height, mine), bf16),
            pltpu.VMEM((2, height, mine), bf16),
            pltpu.VMEM((2, height, mine), bf16),
            pltpu.VMEM((2, 2 * tiles, ROWS, LANES), f32),
            pltpu.VMEM((2, tiles, ROWS, LANES), f32),
            pltpu.VMEM((2, tiles, ROWS, LANES), f32),
            pltpu.VMEM((2, tiles, ROWS, LANES), bf16),
            pltpu.VMEM((2, group - 1, piece, ROWS, LANES), bf16),
            pltpu.VMEM((2, piece, ROWS, LANES), bf16),
            pltpu.VMEM((2, parts, piece, ROWS, LANES), bf16),
            pltpu.VMEM((2, 2 * tiles, ROWS, LANES), bf16),
            pltpu.VMEM((9, 4 * chans, LANES), bf16),
            pltpu.VMEM((9, 4 * chans, LANES), bf16),
            pltpu.VMEM((9, 4 * chans, LANES), bf16),
            pltpu.VMEM((3, 3 * LANES, 4 * chans), f32),
            dma((9,)),
            dma((2, parts - 1)),
            dma((2, parts - 1)),
            dma((3, parts - 1)),
            dma((3, parts - 1)),
            dma((2, 2)),
            dma((2, 2)),
            dma((2, 2, group - 1)),
            dma((2, 2, group - 1)),
            dma((2, parts - 1)),
            dma((2, parts - 1)),
        ],
        compiler_params=pltpu.CompilerParams(
            collective_id=0, has_side_effects=True, vmem_limit_bytes=60 * 1024 * 1024
        ),
        name="block_backward",
    )(
        block_input,
        input_cache,
        middle_cache,
        cotangent,
        first_weight.reshape(27, chans, chans),
        second_weight.reshape(27, chans, chans),
        first_bias,
    )
    results = outs[:3]
    outs = pl.pallas_call(
        functools.partial(finish, plan),
        out_shape=tuple(jax.ShapeDtypeStruct(a.shape, a.dtype) for a in results)
        + (weight_shape,) * 2,
        in_specs=[any_spec] * 3 + [vmem_spec],
        out_specs=(any_spec,) * 3 + (vmem_spec,) * 2,
        scratch_shapes=[pltpu.VMEM(a.shape, a.dtype) for a in results] + [dma((2, 3))],
        name="finish",
    )(*outs)
    grad, x_cache_grad, mid_cache_grad, first_grad, second_grad = outs
    if not plan["direct"]:
        x_cache_grad, mid_cache_grad = (
            lax.all_to_all(a, "tm", split_axis=2, concat_axis=3, tiled=True)
            for a in (x_cache_grad, mid_cache_grad)
        )
    shape = first_weight.shape
    return (
        grad,
        x_cache_grad,
        mid_cache_grad,
        first_grad.reshape(shape),
        second_grad.reshape(shape),
    )


def solution(mesh):
    return jax.shard_map(
        functools.partial(body, dict(mesh.shape)),
        mesh=mesh,
        in_specs=(
            P("clip", "tm", None, None),
            P("clip", None, None, None),
            P("clip", None, None, None),
            P(),
            P(),
            P(),
            P("clip", "tm", None, None),
        ),
        out_specs=(
            P("clip", "tm", None, None),
            P("clip", None, "tm", None),
            P("clip", None, "tm", None),
            P(),
            P(),
        ),
        check_vma=False,
    )
```

```python
import functools
import math

import jax
import jax.numpy as jnp
from jax import lax
from jax.experimental import pallas as pl
from jax.experimental.pallas import tpu as pltpu
from jax.sharding import PartitionSpec as P


def group_of(chans, width):
    group = max(1, 128 // chans)
    return group if width % group == 0 else 1


def bands_with_halo(array, axis, halo):
    count = lax.axis_size(axis)
    band = array.shape[2] // count
    padded = jnp.pad(array, ((0, 0), (0, 0), (halo, halo), (0, 0)))
    pieces = [
        lax.slice_in_dim(padded, p * band, p * band + band + 2 * halo, axis=2)
        for p in range(count)
    ]
    return lax.all_to_all(
        jnp.concatenate(pieces, axis=2), axis, split_axis=2, concat_axis=1, tiled=True
    )


def grouped(array, lanes):
    return array.reshape(array.shape[:-1] + (array.shape[-1] // lanes, lanes))


def patches(array, chans):
    zero = ((0, 0), (0, 0), (0, 0))
    before = jnp.pad(array[:, :, :, :-1, -chans:], zero + ((1, 0), (0, 0)))
    after = jnp.pad(array[:, :, :, 1:, :chans], zero + ((0, 1), (0, 0)))
    window = jnp.concatenate([before, array, after], axis=-1)
    rows = array.shape[2] - 2
    return jnp.concatenate([window[:, :, k : k + rows] for k in range(3)], axis=-1)


def matrix_of(weight, group):
    taps = jnp.transpose(weight, (1, 2, 3, 0, 4))
    zero = (0, 0)
    placed = jnp.stack(
        [jnp.pad(taps, (zero, (p, group - 1 - p), zero, zero, zero)) for p in range(group)],
        axis=4,
    )
    return placed.reshape(
        placed.shape[0] * placed.shape[1] * placed.shape[2], -1
    )


def product(source, matrix):
    return lax.dot_general(
        source, matrix, (((source.ndim - 1,), (0,)), ((), ())), preferred_element_type=jnp.float32
    )


def correlate(left, right):
    axes = tuple(range(left.ndim - 1))
    return lax.dot_general(
        left, right, ((axes, axes), ((), ())), preferred_element_type=jnp.float32
    )


def taps_of(block, group, first, second):
    block = block.reshape(3, group + 2, first, 3, group, second)
    total = None
    for p in range(group):
        part = block[:, p : p + 3, :, :, p, :]
        total = part if total is None else total + part
    return total


def silu_slope(value):
    logistic = jax.nn.sigmoid(value)
    return logistic * (1.0 + value * (1.0 - logistic))


def plain_body(
    block_input, input_cache, middle_cache, first_weight, first_bias, second_weight, cotangent
):
    chans = first_weight.shape[3]
    width = block_input.shape[3] // chans
    group = group_of(chans, width)
    lanes = group * chans
    height = block_input.shape[2]
    parts = lax.axis_size("tm")
    band = height // parts
    offset = lax.axis_index("tm") * band
    count = (
        block_input.shape[0] * lax.axis_size("clip") * block_input.shape[1] * parts * height * width
    )
    factor = 1.0 / math.sqrt(count)

    source = bands_with_halo(block_input, "tm", 2)
    upstream = grouped(bands_with_halo(cotangent, "tm", 2), lanes)
    padded_cache = jnp.pad(input_cache, ((0, 0), (0, 0), (2, 2), (0, 0)))
    cache_in = lax.dynamic_slice_in_dim(padded_cache, offset, band + 4, 2)
    cache_mid = grouped(lax.dynamic_slice_in_dim(middle_cache, offset, band, 2), lanes)
    extended = grouped(jnp.concatenate([cache_in, source], axis=1), lanes)
    frames = upstream.shape[1]

    activated = jax.nn.silu(extended.astype(jnp.float32)).astype(jnp.bfloat16)
    activated_patches = patches(activated, chans)
    forward = product(activated_patches, matrix_of(first_weight, group))
    pre = jnp.tile(first_bias, group)
    for kt in range(3):
        pre = pre + forward[:, kt : kt + frames, ..., kt * lanes : (kt + 1) * lanes]
    middle = jax.nn.silu(pre[:, :, 1:-1]).astype(jnp.bfloat16)
    middle_ext = jnp.concatenate([cache_mid, middle], axis=1)

    upstream_patches = patches(upstream, chans)
    middle_taps = jnp.concatenate(
        [middle_ext[:, kt : kt + frames] for kt in range(3)], axis=-1
    )
    second_block = correlate(upstream_patches[:, :, 1:-1], middle_taps)
    second_sum = taps_of(second_block, group, chans, chans) * factor
    second_sum = jnp.transpose(jnp.flip(second_sum, (0, 1)), (3, 0, 1, 4, 2))
    second_sum, upstream_patches = lax.optimization_barrier(
        (second_sum.reshape(-1, lanes), upstream_patches)
    )

    def input_grad_of(source_patches, weight):
        flipped = jnp.transpose(jnp.flip(weight, (1, 2)), (0, 1, 2, 4, 3))
        result = product(source_patches, matrix_of(flipped, group))
        total = None
        for kt in range(3):
            part = jnp.pad(
                result[..., kt * lanes : (kt + 1) * lanes],
                ((0, 0), (kt, 2 - kt), (0, 0), (0, 0), (0, 0)),
            )
            total = part if total is None else total + part
        return total

    middle_ext_grad = input_grad_of(upstream_patches, second_weight)
    row = offset - 1 + lax.broadcasted_iota(jnp.int32, (band + 2, 1, 1), 0)
    inside = (row >= 0) & (row < height)
    pre_grad = jnp.where(inside, middle_ext_grad[:, 2:] * silu_slope(pre), 0.0)
    pre_grad = pre_grad.astype(jnp.bfloat16)

    own_rows = pre_grad[:, :, 1:-1]
    grad_taps = jnp.concatenate(
        [
            jnp.pad(own_rows, ((0, 0), (kt, 2 - kt), (0, 0), (0, 0), (0, 0)))
            for kt in range(3)
        ],
        axis=-1,
    )
    first_block = correlate(activated_patches[:, :, 1:-1], grad_taps)
    first_sum = taps_of(first_block, group, chans, chans) * factor
    first_sum = jnp.transpose(first_sum, (3, 0, 1, 2, 4))
    first_sum, pre_grad = lax.optimization_barrier((first_sum.reshape(-1, lanes), pre_grad))
    first_total, second_total = lax.optimization_barrier(
        lax.psum((first_sum, second_sum), ("clip", "tm"))
    )

    activated_grad = input_grad_of(patches(pre_grad, chans), first_weight)
    own = extended[:, :, 2:-2].astype(jnp.float32)
    extended_grad = activated_grad * silu_slope(own)
    own_grad = upstream[:, :, 2:-2].astype(jnp.float32) + extended_grad[:, 2:]

    def merged(array):
        return array.astype(jnp.bfloat16).reshape(array.shape[:3] + (width * chans,))

    input_grad = lax.all_to_all(merged(own_grad), "tm", split_axis=1, concat_axis=2, tiled=True)
    return (
        input_grad,
        merged(extended_grad[:, :2]),
        merged(middle_ext_grad[:, :2, 1:-1]),
        first_total.reshape(first_weight.shape),
        second_total.reshape(second_weight.shape),
    )


LANES = 128
ROWS = 16
MESH = pl.DeviceIdType.MESH


def plan_of(sizes, block_input, first_weight):
    chans = first_weight.shape[3]
    parts, clips = sizes["tm"], sizes["clip"]
    local = block_input.shape[1]
    height = block_input.shape[2]
    total = block_input.shape[3] // LANES
    own = total // parts
    held = min(own + (1 if parts == 2 else 2), total)
    taps = 27 * chans // 2 // ROWS
    rest = clips // 2
    merged = rest * parts <= 8
    group = rest * parts if merged else rest
    piece = -(-(taps // 2) // group)
    fits = (
        2 * chans == LANES
        and height % 32 == 0
        and total % parts == 0
        and clips % 2 == 0
        and rest > 1
        and parts > 1
        and local % 2 == 0
        and taps % 2 == 0
    )
    return dict(
        fits=fits,
        chans=chans,
        parts=parts,
        clips=clips,
        local=local,
        frames=local * parts,
        height=height,
        total=total,
        own=own,
        held=held,
        taps=taps,
        rest=rest,
        merged=merged,
        group=group,
        piece=piece,
        band=height // parts,
        direct=(height // parts) % ROWS == 0,
    )


def kernel(
    plan,
    factor,
    x_ref,
    x_cache_ref,
    mid_cache_ref,
    cot_ref,
    first_hbm_ref,
    second_hbm_ref,
    bias_hbm_ref,
    grad_ref,
    x_cache_grad_ref,
    mid_cache_grad_ref,
    gathered_ref,
    ext,
    cot,
    mid_cache,
    act_taps,
    cot_taps,
    pre_taps,
    slope,
    middle,
    middle_t,
    pre_t,
    staged,
    grad_out,
    x_cache_out,
    mid_cache_out,
    sums,
    sums_in,
    wire_own,
    wire,
    wire_in,
    piece_out,
    piece_in,
    gathered,
    first_ref,
    second_back_ref,
    first_back_ref,
    second_acc,
    first_weight_ref,
    second_weight_ref,
    bias_ref,
    local_sem,
    ex_send,
    ex_recv,
    out_send,
    out_recv,
    core_send,
    core_recv,
    ring_send,
    ring_recv,
    part_send,
    part_recv,
):
    chans, parts, local, frames = plan["chans"], plan["parts"], plan["local"], plan["frames"]
    height, own, held, rest = plan["height"], plan["own"], plan["held"], plan["rest"]
    group, merged = plan["group"], plan["merged"]
    piece, band, taps = plan["piece"], plan["band"], plan["taps"]
    half_tiles = group * piece
    filled = taps // 2
    width = held * LANES
    me = lax.axis_index("tm")
    clip = lax.axis_index("clip")
    core = lax.rem(clip, 2)
    chip = clip // 2

    def first_group(index):
        return jnp.minimum(jnp.maximum(index * own - 1, 0), plan["total"] - held)

    def partner(step):
        return lax.rem(me + step, parts)

    rank = me * rest + chip if merged else chip

    def peer(step):
        there = lax.rem(rank + step, group)
        if merged:
            return there, {"clip": lax.rem(there, rest) * 2 + core, "tm": there // rest}
        return there, {"clip": there * 2 + core}

    core_peer = {"clip": clip + 1 - 2 * core}

    begin = first_group(me)
    offset = me * own - begin
    lane0 = pl.multiple_of(begin * LANES, LANES)
    own_lane = pl.multiple_of(me * own * LANES, LANES)

    locals_in = [
        pltpu.make_async_copy(
            x_ref.at[0, :, :, pl.ds(lane0, width)],
            ext.at[pl.ds(2 + me * local, local)],
            local_sem.at[0],
        ),
        pltpu.make_async_copy(
            x_cache_ref.at[0, :, :, pl.ds(lane0, width)], ext.at[pl.ds(0, 2)], local_sem.at[1]
        ),
        pltpu.make_async_copy(
            cot_ref.at[0, :, :, pl.ds(lane0, width)],
            cot.at[pl.ds(me * local, local)],
            local_sem.at[2],
        ),
        pltpu.make_async_copy(
            mid_cache_ref.at[0, :, :, pl.ds(own_lane, own * LANES)], mid_cache, local_sem.at[3]
        ),
    ]
    locals_in += [
        pltpu.make_async_copy(first_hbm_ref, first_weight_ref, local_sem.at[4]),
        pltpu.make_async_copy(second_hbm_ref, second_weight_ref, local_sem.at[5]),
        pltpu.make_async_copy(bias_hbm_ref, bias_ref, local_sem.at[6]),
    ]
    for copy in locals_in:
        copy.start()

    barrier = pltpu.get_barrier_semaphore()
    greeted = [core_peer] + [peer(step)[1] for step in range(1, group)]
    if not merged:
        greeted += [{"tm": partner(step)} for step in range(1, parts)]
    for there in greeted:
        pl.semaphore_signal(barrier, inc=1, device_id=there, device_id_type=MESH)
    pl.semaphore_wait(barrier, len(greeted))

    def exchange(index, source, target, base):
        copies = []
        for step in range(1, parts):
            there = partner(step)
            lane = pl.multiple_of(first_group(there) * LANES, LANES)
            copies.append(
                pltpu.make_async_remote_copy(
                    src_ref=source.at[0, :, :, pl.ds(lane, width)],
                    dst_ref=target.at[pl.ds(base + me * local, local)],
                    send_sem=ex_send.at[index, step - 1],
                    recv_sem=ex_recv.at[index, step - 1],
                    device_id={"tm": there},
                    device_id_type=MESH,
                )
            )
        for copy in copies:
            copy.start()
        return copies

    x_copies = exchange(0, x_ref, ext, 2)
    cot_copies = exchange(1, cot_ref, cot, 0)

    lane_of = lax.broadcasted_iota(jnp.int32, ((held + 1) * height, LANES), 1)
    row_of = lax.rem(
        lax.broadcasted_iota(jnp.int32, ((held + 1) * height, LANES), 0), height
    )

    def put_taps(target, frame, value):
        turned = pltpu.roll(value, chans, 1)
        zero = jnp.zeros((height, LANES), jnp.float32)
        moved = jnp.where(
            lane_of < chans,
            jnp.concatenate([zero, turned], axis=0),
            jnp.concatenate([turned, zero], axis=0),
        )
        count = moved.shape[0]
        above = jnp.where(row_of == 0, 0.0, pltpu.roll(moved, 1, 0))
        below = jnp.where(row_of == height - 1, 0.0, pltpu.roll(moved, count - 1, 0))
        for place, part in enumerate((above, moved, below)):
            target[place, frame] = part.astype(jnp.bfloat16).reshape(held + 1, height, LANES)

    def tiles_of(ref, frame):
        return jnp.concatenate(
            [ref[frame, :, l * LANES : (l + 1) * LANES] for l in range(held)], axis=0
        ).astype(jnp.float32)

    def logistic_of(value):
        return 1.0 / (1.0 + jnp.exp(-value))

    def slope_of(value):
        logistic = logistic_of(value)
        return logistic * (1.0 + value * (1.0 - logistic))

    def put_act(frame):
        value = tiles_of(ext, frame)
        put_taps(act_taps, frame, value * logistic_of(value))

    def put_cot(frame):
        put_taps(cot_taps, frame, tiles_of(cot, frame))

    def loop(count, call):
        def step(index, carry):
            call(index)
            return carry

        lax.fori_loop(0, count, step, 0)

    def window(ref, place, frame, start, count):
        left = ref[place, frame, pl.ds(start, count)].reshape(count * height, LANES)
        right = ref[place, frame, pl.ds(start + 1, count)].reshape(count * height, LANES)
        return jnp.concatenate([left, right], axis=1)

    def matrix(ref, early, late, place):
        zero = jnp.zeros((4 * chans, LANES), jnp.bfloat16)
        parts_of = [zero if k is None else ref[k * 3 + place] for k in (early, late)]
        return jnp.concatenate(parts_of, axis=1)

    def pair_product(ref, base, used, start, count, weight_ref, taps_at):
        total = None
        for f in used:
            early, late = taps_at(f)
            for place in range(3):
                part = jnp.dot(
                    window(ref, place, base + f, start, count),
                    matrix(weight_ref, early, late, place),
                    preferred_element_type=jnp.float32,
                )
                total = part if total is None else total + part
        return total

    def inside(k):
        return k if 0 <= k <= 2 else None

    def ahead(f):
        return inside(f), inside(f - 1)

    def behind(f):
        return inside(2 - f), inside(3 - f)

    locals_in[0].wait()
    locals_in[1].wait()
    loop(2, put_act)
    loop(local, lambda f: put_act(2 + me * local + f))
    locals_in[2].wait()
    loop(local, lambda f: put_cot(me * local + f))
    locals_in[3].wait()

    def put_cache(frame):
        joined = jnp.concatenate(
            [mid_cache[frame, :, l * LANES : (l + 1) * LANES] for l in range(own)], axis=0
        )
        middle_t[frame] = jnp.transpose(joined)

    loop(2, put_cache)

    def strip(target, at, pieces):
        none = jnp.zeros((chans, chans), jnp.bfloat16)
        for place in range(4):
            left = pieces[place] if place < 3 else none
            right = pieces[place - 1] if place > 0 else none
            target[at, place * chans : (place + 1) * chans] = jnp.concatenate(
                [left, right], axis=1
            )

    def put_strips(index):
        strip(first_ref, index, [first_weight_ref[index * 3 + kq] for kq in range(3)])
        flipped = (index // 3 * 3 + 2 - lax.rem(index, 3)) * 3 + 2
        for target, source in (
            (second_back_ref, second_weight_ref),
            (first_back_ref, first_weight_ref),
        ):
            strip(target, index, [jnp.transpose(source[flipped - kq]) for kq in range(3)])

    locals_in[4].wait()
    locals_in[5].wait()
    locals_in[6].wait()
    loop(9, put_strips)

    for step, copy in enumerate(x_copies):
        copy.wait_recv()
        there = lax.rem(me + parts - step - 1, parts)
        loop(local, lambda f: put_act(2 + there * local + f))

    bias = bias_ref[...].reshape(1, chans)
    bias = jnp.concatenate([bias] * (LANES // chans), axis=1)

    def forward(pair):
        base = 2 * pair
        total = pair_product(act_taps, base, range(4), 0, held, first_ref, ahead)
        for u in range(2):
            pre = total[:, u * LANES : (u + 1) * LANES] + bias
            logistic = logistic_of(pre)
            slope[base + u] = logistic * (1.0 + pre * (1.0 - logistic))
            middle[base + u] = (pre * logistic).astype(jnp.bfloat16).reshape(held, height, LANES)
            mine = middle[base + u, pl.ds(offset, own)].reshape(own * height, LANES)
            middle_t[2 + base + u] = jnp.transpose(mine)

    loop(frames // 2, forward)

    def second_part(block, fresh):
        def at(place):
            total = None
            for f in range(local):
                frame = block * local + f
                left = middle_t[pl.ds(frame, 3)].reshape(3 * LANES, own * height)
                part = jnp.dot(
                    left,
                    window(cot_taps, place, frame, offset, own),
                    preferred_element_type=jnp.float32,
                )
                total = part if total is None else total + part
            second_acc[place] = total if fresh else second_acc[place] + total

        loop(3, at)

    second_part(me, True)
    for step, copy in enumerate(cot_copies):
        copy.wait_recv()
        there = lax.rem(me + parts - step - 1, parts)
        loop(local, lambda f: put_cot(there * local + f))
        second_part(there, False)

    half_lane = lax.broadcasted_iota(jnp.int32, (chans // 2, LANES), 1)

    def put_sum(which, index, value):
        value = value[:chans] + pltpu.roll(value[chans:], 3 * chans, 1)
        value = value * factor
        low, high = value[:, :LANES], value[:, LANES:]
        half = chans // 2
        tail = jnp.where(half_lane < chans, high[:half], pltpu.roll(high[half:], chans, 1))
        rows = jnp.concatenate([low, tail], axis=0)
        for n in range(3 * chans // 2 // ROWS):
            tile = index * (3 * chans // 2 // ROWS) + n
            tile = tile + (half_tiles - filled) * (tile // filled)
            sums[which, tile] = rows[n * ROWS : (n + 1) * ROWS]

    def put_second(place):
        value = second_acc[place]
        for kt in range(3):
            put_sum(0, kt * 3 + place, value[kt * LANES : (kt + 1) * LANES])

    mine = core * half_tiles
    other = (1 - core) * half_tiles
    whole = mine + rank * piece
    core_copies, ring, across, spread, last = [], [], [], [], []

    def swap_cores(which):
        for h in range(2):
            for n in range(filled, half_tiles):
                sums[which, h * half_tiles + n] = jnp.zeros((ROWS, LANES), jnp.float32)
        core_copies.append(
            pltpu.make_async_remote_copy(
                src_ref=sums.at[which, pl.ds(other, half_tiles)],
                dst_ref=sums_in.at[which],
                send_sem=core_send.at[0, which],
                recv_sem=core_recv.at[0, which],
                device_id=core_peer,
                device_id_type=MESH,
            )
        )
        core_copies[-1].start()

    def scatter(which):
        core_copies[which].wait_recv()

        def chip_sum(index):
            total = sums[which, mine + index] + sums_in[which, index]
            wire_own[which, index] = total
            wire[which, index] = total.astype(jnp.bfloat16)

        loop(half_tiles, chip_sum)
        copies = []
        for step in range(1, group):
            there, device = peer(step)
            copies.append(
                pltpu.make_async_remote_copy(
                    src_ref=wire.at[which, pl.ds(there * piece, piece)],
                    dst_ref=wire_in.at[which, step - 1],
                    send_sem=ring_send.at[0, which, step - 1],
                    recv_sem=ring_recv.at[0, which, step - 1],
                    device_id=device,
                    device_id_type=MESH,
                )
            )
        for copy in copies:
            copy.start()
        ring.append(copies)

    def gather(which):
        for copy in ring[which]:
            copy.wait_recv()

        def slice_sum(index):
            total = wire_own[which, rank * piece + index]
            for step in range(1, group):
                total = total + wire_in[which, step - 1, index].astype(jnp.float32)
            piece_out[which, index] = total.astype(jnp.bfloat16)

        loop(piece, slice_sum)
        if merged:
            gathered[which, pl.ds(whole, piece)] = piece_out[which]
        else:
            copies = []
            for step in range(1, parts):
                copies.append(
                    pltpu.make_async_remote_copy(
                        src_ref=piece_out.at[which],
                        dst_ref=piece_in.at[which, me],
                        send_sem=part_send.at[which, step - 1],
                        recv_sem=part_recv.at[which, step - 1],
                        device_id={"tm": partner(step)},
                        device_id_type=MESH,
                    )
                )
            for copy in copies:
                copy.start()
            across.extend(copies)
            piece_in[which, me] = piece_out[which]
            for copy in copies:
                copy.wait_recv()

            def part_sum(index):
                total = piece_in[which, 0, index].astype(jnp.float32)
                for p in range(1, parts):
                    total = total + piece_in[which, p, index].astype(jnp.float32)
                gathered[which, whole + index] = total.astype(jnp.bfloat16)

            loop(piece, part_sum)
        copies = []
        for step in range(1, group):
            copies.append(
                pltpu.make_async_remote_copy(
                    src_ref=gathered.at[which, pl.ds(whole, piece)],
                    dst_ref=gathered.at[which, pl.ds(whole, piece)],
                    send_sem=ring_send.at[1, which, step - 1],
                    recv_sem=ring_recv.at[1, which, step - 1],
                    device_id=peer(step)[1],
                    device_id_type=MESH,
                )
            )
        for copy in copies:
            copy.start()
        spread.append(copies)

    def share(which):
        for copy in spread[which]:
            copy.wait_recv()
        last.append(
            pltpu.make_async_remote_copy(
                src_ref=gathered.at[which, pl.ds(mine, half_tiles)],
                dst_ref=gathered.at[which, pl.ds(mine, half_tiles)],
                send_sem=core_send.at[1, which],
                recv_sem=core_recv.at[1, which],
                device_id=core_peer,
                device_id_type=MESH,
            )
        )
        last[-1].start()

    loop(3, put_second)
    swap_cores(0)

    def lay_out(target, frame, u):
        for l in range(own):
            target[frame, :, l * LANES : (l + 1) * LANES] = staged[u, offset + l].astype(
                target.dtype
            )

    first_pair = pair_product(cot_taps, -2, range(2, 4), 0, held, second_back_ref, behind)
    for u in range(2):
        staged[u] = first_pair[:, u * LANES : (u + 1) * LANES].reshape(held, height, LANES)
    for u in range(2):
        lay_out(mid_cache_out, u, u)

    def send_out(slot, source_of, target):
        copies = []
        for step in range(1, parts):
            there = partner(step)
            copies.append(
                pltpu.make_async_remote_copy(
                    src_ref=source_of(there),
                    dst_ref=target,
                    send_sem=out_send.at[slot, step - 1],
                    recv_sem=out_recv.at[slot, step - 1],
                    device_id={"tm": there},
                    device_id_type=MESH,
                )
            )
            copies[-1].start()
        outgoing.extend(copies)

    own_lanes = pl.ds(own_lane, own * LANES)

    def band_rows(index):
        return pl.ds(pl.multiple_of(index * band, ROWS), band)

    def send_cache(slot, source, target):
        if plan["direct"]:
            send_out(
                slot,
                lambda there: source.at[:, band_rows(there), :],
                target.at[0, :, :, own_lanes],
            )
            target[0, :, :, own_lanes] = source[:, band_rows(me), :]
        else:
            target[0] = source[...]

    outgoing = []
    scatter(0)
    send_cache(0, mid_cache_out, mid_cache_grad_ref)

    def put_pre(total, base):
        for u in range(2):
            grad = total[:, u * LANES : (u + 1) * LANES] * slope[base + u]
            put_taps(pre_taps, base + u, grad)
            at = frames + base + u
            middle[at] = grad.astype(jnp.bfloat16).reshape(held, height, LANES)
            mine = middle[at, pl.ds(offset, own)].reshape(own * height, LANES)
            pre_t[base + u] = jnp.transpose(mine)

    def inner_pair(pair):
        base = 2 * pair
        put_pre(
            pair_product(cot_taps, base, range(4), 0, held, second_back_ref, behind), base
        )

    loop(frames // 2 - 1, inner_pair)
    put_pre(
        pair_product(cot_taps, frames - 2, range(2), 0, held, second_back_ref, behind),
        frames - 2,
    )

    def first_at(place):
        totals = [None] * 3
        for m in range(frames + 2):
            t0, t1 = max(0, m - 2), min(frames - 1, m)
            count = t1 - t0 + 1
            part = jnp.dot(
                pre_t[t0 : t1 + 1].reshape(count * LANES, own * height),
                window(act_taps, place, m, offset, own),
                preferred_element_type=jnp.float32,
            )
            for t in range(t0, t1 + 1):
                piece_of = part[(t - t0) * LANES : (t - t0 + 1) * LANES]
                kt = m - t
                totals[kt] = piece_of if totals[kt] is None else totals[kt] + piece_of
        for kt in range(3):
            put_sum(1, kt * 3 + place, totals[kt])

    loop(3, first_at)
    swap_cores(1)

    def put_ext(total, base, cached):
        for u in range(2):
            for l in range(own):
                lane = pl.multiple_of((offset + l) * LANES, LANES)
                value = ext[base + u, :, pl.ds(lane, LANES)].astype(jnp.float32)
                grad = (
                    total[l * height : (l + 1) * height, u * LANES : (u + 1) * LANES]
                    * slope_of(value)
                )
                place = slice(l * LANES, (l + 1) * LANES)
                if cached:
                    x_cache_out[base + u, :, place] = grad.astype(jnp.bfloat16)
                else:
                    given = cot[base + u - 2, :, pl.ds(lane, LANES)].astype(jnp.float32)
                    grad_out[base + u - 2, :, place] = (given + grad).astype(jnp.bfloat16)

    put_ext(
        pair_product(pre_taps, -2, range(2, 4), offset, own, first_back_ref, behind), 0, True
    )
    scatter(1)

    def send_grad(f):
        send_out(
            2 + f,
            lambda there: grad_out.at[there * local + f],
            grad_ref.at[0, f, :, own_lanes],
        )
        grad_ref[0, f, :, own_lanes] = grad_out[me * local + f]

    def inner_ext(pair):
        base = 2 * pair
        put_ext(
            pair_product(pre_taps, base - 2, range(4), offset, own, first_back_ref, behind),
            base,
            False,
        )

    for pair in range(1, frames // 2):
        inner_ext(pair)
    put_ext(
        pair_product(pre_taps, frames - 2, range(2), offset, own, first_back_ref, behind),
        frames,
        False,
    )
    gather(0)
    send_cache(1, x_cache_out, x_cache_grad_ref)
    send_grad(0)
    gather(1)
    for f in range(1, local):
        send_grad(f)
    share(0)
    share(1)
    for which in range(2):
        last[which].wait_recv()
    gathered_ref[...] = gathered[...]

    for copy in outgoing:
        copy.wait()
    for copy in x_copies + cot_copies + core_copies + across + last:
        copy.wait_send()
    for copies in ring + spread:
        for copy in copies:
            copy.wait_send()


def finish(plan, *refs):
    sources, gathered, targets = refs[:3], refs[3], refs[4:9]
    first, second, sems = refs[9:]
    chans, taps = plan["chans"], plan["taps"]
    filled, half_tiles = taps // 2, plan["group"] * plan["piece"]
    leaving = [
        pltpu.make_async_copy(source, target, sems.at[n])
        for n, (source, target) in enumerate(zip(sources + (first, second), targets))
    ]
    for copy in leaving[:3]:
        copy.start()

    def rows_of(which, index):
        tiles = []
        for n in range(3 * chans // 2 // ROWS):
            tile = index * (3 * chans // 2 // ROWS) + n
            tiles.append(gathered[which, tile + (half_tiles - filled) * (tile // filled)])
        rows = jnp.concatenate(tiles, axis=0).astype(jnp.float32)
        tail = jnp.concatenate([rows[chans:, :chans], rows[chans:, chans:]], axis=0)
        return rows[:chans, :chans], rows[:chans, chans:], tail

    def second_step(index, carry):
        kt, place = index // 3, lax.rem(index, 3)
        for kq, value in enumerate(rows_of(0, index)):
            second[(kt * 3 + 2 - place) * 3 + 2 - kq] = value
        return carry

    def first_step(index, carry):
        for kq, value in enumerate(rows_of(1, index)):
            first[index * 3 + kq] = jnp.transpose(value)
        return carry

    lax.fori_loop(0, 9, second_step, 0)
    leaving[4].start()
    lax.fori_loop(0, 9, first_step, 0)
    leaving[3].start()
    for copy in leaving:
        copy.wait()


def body(sizes, *arrays):
    (
        block_input,
        input_cache,
        middle_cache,
        first_weight,
        first_bias,
        second_weight,
        cotangent,
    ) = arrays
    plan = plan_of(sizes, block_input, first_weight)
    if not plan["fits"]:
        return plain_body(*arrays)
    chans, parts, local, frames = plan["chans"], plan["parts"], plan["local"], plan["frames"]
    height, own, held, rest = plan["height"], plan["own"], plan["held"], plan["rest"]
    piece, band, total = plan["piece"], plan["band"], plan["total"]
    count = block_input.shape[0] * plan["clips"] * frames * height * total * LANES // chans
    factor = 1.0 / math.sqrt(count)
    wide, mine = held * LANES, own * LANES
    group = plan["group"]
    tiles = group * piece
    bf16, f32 = jnp.bfloat16, jnp.float32
    if plan["direct"]:
        cache_shape = (1, 2, band, total * LANES)
    else:
        cache_shape = (1, 2, height, mine)
    hbm_spec = pl.BlockSpec(memory_space=pltpu.HBM)
    vmem_spec = pl.BlockSpec(memory_space=pltpu.VMEM)
    dma = pltpu.SemaphoreType.DMA
    weight_shape = jax.ShapeDtypeStruct((27, chans, chans), f32)
    outs = pl.pallas_call(
        functools.partial(kernel, plan, factor),
        out_shape=(
            jax.ShapeDtypeStruct(block_input.shape, bf16),
            jax.ShapeDtypeStruct(cache_shape, bf16),
            jax.ShapeDtypeStruct(cache_shape, bf16),
            jax.ShapeDtypeStruct((2, 2 * tiles, ROWS, LANES), bf16),
        ),
        in_specs=[hbm_spec] * 7,
        out_specs=(vmem_spec,) * 4,
        scratch_shapes=[
            pltpu.VMEM((frames + 2, height, wide), bf16),
            pltpu.VMEM((frames, height, wide), bf16),
            pltpu.VMEM((2, height, mine), bf16),
            pltpu.VMEM((3, frames + 2, held + 1, height, LANES), bf16),
            pltpu.VMEM((3, frames, held + 1, height, LANES), bf16),
            pltpu.VMEM((3, frames, held + 1, height, LANES), bf16),
            pltpu.VMEM((frames, held * height, LANES), f32),
            pltpu.VMEM((2 * frames, held, height, LANES), bf16),
            pltpu.VMEM((frames + 2, LANES, own * height), bf16),
            pltpu.VMEM((frames, LANES, own * height), bf16),
            pltpu.VMEM((2, held, height, LANES), f32),
            pltpu.VMEM((frames, height, mine), bf16),
            pltpu.VMEM((2, height, mine), bf16),
            pltpu.VMEM((2, height, mine), bf16),
            pltpu.VMEM((2, 2 * tiles, ROWS, LANES), f32),
            pltpu.VMEM((2, tiles, ROWS, LANES), f32),
            pltpu.VMEM((2, tiles, ROWS, LANES), f32),
            pltpu.VMEM((2, tiles, ROWS, LANES), bf16),
            pltpu.VMEM((2, group - 1, piece, ROWS, LANES), bf16),
            pltpu.VMEM((2, piece, ROWS, LANES), bf16),
            pltpu.VMEM((2, parts, piece, ROWS, LANES), bf16),
            pltpu.VMEM((2, 2 * tiles, ROWS, LANES), bf16),
            pltpu.VMEM((9, 4 * chans, LANES), bf16),
            pltpu.VMEM((9, 4 * chans, LANES), bf16),
            pltpu.VMEM((9, 4 * chans, LANES), bf16),
            pltpu.VMEM((3, 3 * LANES, 4 * chans), f32),
            pltpu.VMEM((27, chans, chans), bf16),
            pltpu.VMEM((27, chans, chans), bf16),
            pltpu.VMEM((chans,), f32),
            dma((7,)),
            dma((2, parts - 1)),
            dma((2, parts - 1)),
            dma((2 + local, parts - 1)),
            dma((2 + local, parts - 1)),
            dma((2, 2)),
            dma((2, 2)),
            dma((2, 2, group - 1)),
            dma((2, 2, group - 1)),
            dma((2, parts - 1)),
            dma((2, parts - 1)),
        ],
        compiler_params=pltpu.CompilerParams(
            collective_id=0, has_side_effects=True, vmem_limit_bytes=36 * 1024 * 1024
        ),
        name="block_backward",
    )(
        *(
            pltpu.with_memory_space_constraint(a, pltpu.HBM)
            for a in (
                block_input,
                input_cache,
                middle_cache,
                cotangent,
                first_weight.reshape(27, chans, chans),
                second_weight.reshape(27, chans, chans),
                first_bias,
            )
        )
    )
    results = outs[:3]
    outs = pl.pallas_call(
        functools.partial(finish, plan),
        out_shape=tuple(jax.ShapeDtypeStruct(a.shape, a.dtype) for a in results)
        + (weight_shape,) * 2,
        in_specs=[vmem_spec] * 4,
        out_specs=(hbm_spec,) * 5,
        scratch_shapes=[pltpu.VMEM(weight_shape.shape, f32)] * 2 + [dma((5,))],
        compiler_params=pltpu.CompilerParams(vmem_limit_bytes=8 * 1024 * 1024),
        name="finish",
    )(*outs)
    grad, x_cache_grad, mid_cache_grad, first_grad, second_grad = outs
    if not plan["direct"]:
        x_cache_grad, mid_cache_grad = (
            lax.all_to_all(a, "tm", split_axis=2, concat_axis=3, tiled=True)
            for a in (x_cache_grad, mid_cache_grad)
        )
    shape = first_weight.shape
    return (
        grad,
        x_cache_grad,
        mid_cache_grad,
        first_grad.reshape(shape),
        second_grad.reshape(shape),
    )


def solution(mesh):
    return jax.shard_map(
        functools.partial(body, dict(mesh.shape)),
        mesh=mesh,
        in_specs=(
            P("clip", "tm", None, None),
            P("clip", None, None, None),
            P("clip", None, None, None),
            P(),
            P(),
            P(),
            P("clip", "tm", None, None),
        ),
        out_specs=(
            P("clip", "tm", None, None),
            P("clip", None, "tm", None),
            P("clip", None, "tm", None),
            P(),
            P(),
        ),
        check_vma=False,
    )
```

```python
import functools
import math

import jax
import jax.numpy as jnp
from jax import lax
from jax.experimental import pallas as pl
from jax.experimental.pallas import tpu as pltpu
from jax.sharding import PartitionSpec as P


def group_of(chans, width):
    group = max(1, 128 // chans)
    return group if width % group == 0 else 1


def bands_with_halo(array, axis, halo):
    count = lax.axis_size(axis)
    band = array.shape[2] // count
    padded = jnp.pad(array, ((0, 0), (0, 0), (halo, halo), (0, 0)))
    pieces = [
        lax.slice_in_dim(padded, p * band, p * band + band + 2 * halo, axis=2)
        for p in range(count)
    ]
    return lax.all_to_all(
        jnp.concatenate(pieces, axis=2), axis, split_axis=2, concat_axis=1, tiled=True
    )


def grouped(array, lanes):
    return array.reshape(array.shape[:-1] + (array.shape[-1] // lanes, lanes))


def patches(array, chans):
    zero = ((0, 0), (0, 0), (0, 0))
    before = jnp.pad(array[:, :, :, :-1, -chans:], zero + ((1, 0), (0, 0)))
    after = jnp.pad(array[:, :, :, 1:, :chans], zero + ((0, 1), (0, 0)))
    window = jnp.concatenate([before, array, after], axis=-1)
    rows = array.shape[2] - 2
    return jnp.concatenate([window[:, :, k : k + rows] for k in range(3)], axis=-1)


def matrix_of(weight, group):
    taps = jnp.transpose(weight, (1, 2, 3, 0, 4))
    zero = (0, 0)
    placed = jnp.stack(
        [jnp.pad(taps, (zero, (p, group - 1 - p), zero, zero, zero)) for p in range(group)],
        axis=4,
    )
    return placed.reshape(
        placed.shape[0] * placed.shape[1] * placed.shape[2], -1
    )


def product(source, matrix):
    return lax.dot_general(
        source, matrix, (((source.ndim - 1,), (0,)), ((), ())), preferred_element_type=jnp.float32
    )


def correlate(left, right):
    axes = tuple(range(left.ndim - 1))
    return lax.dot_general(
        left, right, ((axes, axes), ((), ())), preferred_element_type=jnp.float32
    )


def taps_of(block, group, first, second):
    block = block.reshape(3, group + 2, first, 3, group, second)
    total = None
    for p in range(group):
        part = block[:, p : p + 3, :, :, p, :]
        total = part if total is None else total + part
    return total


def silu_slope(value):
    logistic = jax.nn.sigmoid(value)
    return logistic * (1.0 + value * (1.0 - logistic))


def plain_body(
    block_input, input_cache, middle_cache, first_weight, first_bias, second_weight, cotangent
):
    chans = first_weight.shape[3]
    width = block_input.shape[3] // chans
    group = group_of(chans, width)
    lanes = group * chans
    height = block_input.shape[2]
    parts = lax.axis_size("tm")
    band = height // parts
    offset = lax.axis_index("tm") * band
    count = (
        block_input.shape[0] * lax.axis_size("clip") * block_input.shape[1] * parts * height * width
    )
    factor = 1.0 / math.sqrt(count)

    source = bands_with_halo(block_input, "tm", 2)
    upstream = grouped(bands_with_halo(cotangent, "tm", 2), lanes)
    padded_cache = jnp.pad(input_cache, ((0, 0), (0, 0), (2, 2), (0, 0)))
    cache_in = lax.dynamic_slice_in_dim(padded_cache, offset, band + 4, 2)
    cache_mid = grouped(lax.dynamic_slice_in_dim(middle_cache, offset, band, 2), lanes)
    extended = grouped(jnp.concatenate([cache_in, source], axis=1), lanes)
    frames = upstream.shape[1]

    activated = jax.nn.silu(extended.astype(jnp.float32)).astype(jnp.bfloat16)
    activated_patches = patches(activated, chans)
    forward = product(activated_patches, matrix_of(first_weight, group))
    pre = jnp.tile(first_bias, group)
    for kt in range(3):
        pre = pre + forward[:, kt : kt + frames, ..., kt * lanes : (kt + 1) * lanes]
    middle = jax.nn.silu(pre[:, :, 1:-1]).astype(jnp.bfloat16)
    middle_ext = jnp.concatenate([cache_mid, middle], axis=1)

    upstream_patches = patches(upstream, chans)
    middle_taps = jnp.concatenate(
        [middle_ext[:, kt : kt + frames] for kt in range(3)], axis=-1
    )
    second_block = correlate(upstream_patches[:, :, 1:-1], middle_taps)
    second_sum = taps_of(second_block, group, chans, chans) * factor
    second_sum = jnp.transpose(jnp.flip(second_sum, (0, 1)), (3, 0, 1, 4, 2))
    second_sum, upstream_patches = lax.optimization_barrier(
        (second_sum.reshape(-1, lanes), upstream_patches)
    )

    def input_grad_of(source_patches, weight):
        flipped = jnp.transpose(jnp.flip(weight, (1, 2)), (0, 1, 2, 4, 3))
        result = product(source_patches, matrix_of(flipped, group))
        total = None
        for kt in range(3):
            part = jnp.pad(
                result[..., kt * lanes : (kt + 1) * lanes],
                ((0, 0), (kt, 2 - kt), (0, 0), (0, 0), (0, 0)),
            )
            total = part if total is None else total + part
        return total

    middle_ext_grad = input_grad_of(upstream_patches, second_weight)
    row = offset - 1 + lax.broadcasted_iota(jnp.int32, (band + 2, 1, 1), 0)
    inside = (row >= 0) & (row < height)
    pre_grad = jnp.where(inside, middle_ext_grad[:, 2:] * silu_slope(pre), 0.0)
    pre_grad = pre_grad.astype(jnp.bfloat16)

    own_rows = pre_grad[:, :, 1:-1]
    grad_taps = jnp.concatenate(
        [
            jnp.pad(own_rows, ((0, 0), (kt, 2 - kt), (0, 0), (0, 0), (0, 0)))
            for kt in range(3)
        ],
        axis=-1,
    )
    first_block = correlate(activated_patches[:, :, 1:-1], grad_taps)
    first_sum = taps_of(first_block, group, chans, chans) * factor
    first_sum = jnp.transpose(first_sum, (3, 0, 1, 2, 4))
    first_sum, pre_grad = lax.optimization_barrier((first_sum.reshape(-1, lanes), pre_grad))
    first_total, second_total = lax.optimization_barrier(
        lax.psum((first_sum, second_sum), ("clip", "tm"))
    )

    activated_grad = input_grad_of(patches(pre_grad, chans), first_weight)
    own = extended[:, :, 2:-2].astype(jnp.float32)
    extended_grad = activated_grad * silu_slope(own)
    own_grad = upstream[:, :, 2:-2].astype(jnp.float32) + extended_grad[:, 2:]

    def merged(array):
        return array.astype(jnp.bfloat16).reshape(array.shape[:3] + (width * chans,))

    input_grad = lax.all_to_all(merged(own_grad), "tm", split_axis=1, concat_axis=2, tiled=True)
    return (
        input_grad,
        merged(extended_grad[:, :2]),
        merged(middle_ext_grad[:, :2, 1:-1]),
        first_total.reshape(first_weight.shape),
        second_total.reshape(second_weight.shape),
    )


LANES = 128
ROWS = 16
MESH = pl.DeviceIdType.MESH


def plan_of(sizes, block_input, first_weight):
    chans = first_weight.shape[3]
    parts, clips = sizes["tm"], sizes["clip"]
    local = block_input.shape[1]
    height = block_input.shape[2]
    total = block_input.shape[3] // LANES
    own = total // parts
    held = min(own + (1 if parts == 2 else 2), total)
    taps = 27 * chans // 2 // ROWS
    rest = clips // 2
    merged = rest * parts <= 8
    group = rest * parts if merged else rest
    piece = -(-(taps // 2) // group)
    fits = (
        2 * chans == LANES
        and height % 32 == 0
        and total % parts == 0
        and clips % 2 == 0
        and rest > 1
        and parts > 1
        and local % 2 == 0
        and taps % 2 == 0
    )
    return dict(
        fits=fits,
        chans=chans,
        parts=parts,
        clips=clips,
        local=local,
        frames=local * parts,
        height=height,
        total=total,
        own=own,
        held=held,
        taps=taps,
        rest=rest,
        merged=merged,
        group=group,
        piece=piece,
        band=height // parts,
        direct=(height // parts) % ROWS == 0,
    )


def kernel(
    plan,
    factor,
    x_ref,
    x_cache_ref,
    mid_cache_ref,
    cot_ref,
    first_hbm_ref,
    second_hbm_ref,
    bias_hbm_ref,
    grad_ref,
    x_cache_grad_ref,
    mid_cache_grad_ref,
    second_grad_ref,
    gathered_ref,
    ext,
    cot,
    mid_cache,
    act_taps,
    cot_taps,
    pre_taps,
    slope,
    middle,
    middle_t,
    pre_t,
    staged,
    grad_out,
    x_cache_out,
    mid_cache_out,
    sums,
    sums_in,
    wire_own,
    wire,
    wire_in,
    piece_out,
    piece_in,
    gathered,
    first_ref,
    second_back_ref,
    first_back_ref,
    second_acc,
    middle_grad,
    first_weight_ref,
    second_weight_ref,
    bias_ref,
    local_sem,
    ex_send,
    ex_recv,
    out_send,
    out_recv,
    core_send,
    core_recv,
    ring_send,
    ring_recv,
    part_send,
    part_recv,
):
    chans, parts, local, frames = plan["chans"], plan["parts"], plan["local"], plan["frames"]
    height, own, held, rest = plan["height"], plan["own"], plan["held"], plan["rest"]
    group, merged = plan["group"], plan["merged"]
    piece, band, taps = plan["piece"], plan["band"], plan["taps"]
    half_tiles = group * piece
    filled = taps // 2
    width = held * LANES
    me = lax.axis_index("tm")
    clip = lax.axis_index("clip")
    core = lax.rem(clip, 2)
    chip = clip // 2

    def first_group(index):
        return jnp.minimum(jnp.maximum(index * own - 1, 0), plan["total"] - held)

    def partner(step):
        return lax.rem(me + step, parts)

    rank = me * rest + chip if merged else chip

    def peer(step):
        there = lax.rem(rank + step, group)
        if merged:
            return there, {"clip": lax.rem(there, rest) * 2 + core, "tm": there // rest}
        return there, {"clip": there * 2 + core}

    core_peer = {"clip": clip + 1 - 2 * core}

    begin = first_group(me)
    offset = me * own - begin
    lane0 = pl.multiple_of(begin * LANES, LANES)
    own_lane = pl.multiple_of(me * own * LANES, LANES)

    locals_in = [
        pltpu.make_async_copy(
            x_ref.at[0, :, :, pl.ds(lane0, width)],
            ext.at[pl.ds(2 + me * local, local)],
            local_sem.at[0],
        ),
        pltpu.make_async_copy(
            x_cache_ref.at[0, :, :, pl.ds(lane0, width)], ext.at[pl.ds(0, 2)], local_sem.at[1]
        ),
        pltpu.make_async_copy(
            cot_ref.at[0, :, :, pl.ds(lane0, width)],
            cot.at[pl.ds(me * local, local)],
            local_sem.at[2],
        ),
        pltpu.make_async_copy(
            mid_cache_ref.at[0, :, :, pl.ds(own_lane, own * LANES)], mid_cache, local_sem.at[3]
        ),
    ]
    locals_in += [
        pltpu.make_async_copy(first_hbm_ref, first_weight_ref, local_sem.at[4]),
        pltpu.make_async_copy(second_hbm_ref, second_weight_ref, local_sem.at[5]),
        pltpu.make_async_copy(bias_hbm_ref, bias_ref, local_sem.at[6]),
    ]
    for copy in locals_in:
        copy.start()

    barrier = pltpu.get_barrier_semaphore()
    greeted = [core_peer] + [peer(step)[1] for step in range(1, group)]
    if not merged:
        greeted += [{"tm": partner(step)} for step in range(1, parts)]
    for there in greeted:
        pl.semaphore_signal(barrier, inc=1, device_id=there, device_id_type=MESH)
    pl.semaphore_wait(barrier, len(greeted))

    def exchange(index, source, target, base):
        copies = []
        for step in range(1, parts):
            there = partner(step)
            lane = pl.multiple_of(first_group(there) * LANES, LANES)
            copies.append(
                pltpu.make_async_remote_copy(
                    src_ref=source.at[0, :, :, pl.ds(lane, width)],
                    dst_ref=target.at[pl.ds(base + me * local, local)],
                    send_sem=ex_send.at[index, step - 1],
                    recv_sem=ex_recv.at[index, step - 1],
                    device_id={"tm": there},
                    device_id_type=MESH,
                )
            )
        for copy in copies:
            copy.start()
        return copies

    x_copies = exchange(0, x_ref, ext, 2)
    cot_copies = exchange(1, cot_ref, cot, 0)

    lane_of = lax.broadcasted_iota(jnp.int32, ((held + 1) * height, LANES), 1)
    row_of = lax.rem(
        lax.broadcasted_iota(jnp.int32, ((held + 1) * height, LANES), 0), height
    )

    def put_taps(target, frame, value):
        turned = pltpu.roll(value, chans, 1)
        zero = jnp.zeros((height, LANES), jnp.float32)
        moved = jnp.where(
            lane_of < chans,
            jnp.concatenate([zero, turned], axis=0),
            jnp.concatenate([turned, zero], axis=0),
        )
        count = moved.shape[0]
        above = jnp.where(row_of == 0, 0.0, pltpu.roll(moved, 1, 0))
        below = jnp.where(row_of == height - 1, 0.0, pltpu.roll(moved, count - 1, 0))
        for place, part in enumerate((above, moved, below)):
            target[place, frame] = part.astype(jnp.bfloat16).reshape(held + 1, height, LANES)

    def tiles_of(ref, frame):
        return jnp.concatenate(
            [ref[frame, :, l * LANES : (l + 1) * LANES] for l in range(held)], axis=0
        ).astype(jnp.float32)

    def logistic_of(value):
        return 1.0 / (1.0 + jnp.exp(-value))

    def slope_of(value):
        logistic = logistic_of(value)
        return logistic * (1.0 + value * (1.0 - logistic))

    def put_act(frame):
        value = tiles_of(ext, frame)
        put_taps(act_taps, frame, value * logistic_of(value))

    def put_cot(frame):
        put_taps(cot_taps, frame, tiles_of(cot, frame))

    def loop(count, call):
        def step(index, carry):
            call(index)
            return carry

        lax.fori_loop(0, count, step, 0)

    def window(ref, place, frame, start, count):
        left = ref[place, frame, pl.ds(start, count)].reshape(count * height, LANES)
        right = ref[place, frame, pl.ds(start + 1, count)].reshape(count * height, LANES)
        return jnp.concatenate([left, right], axis=1)

    def matrix(ref, early, late, place):
        zero = jnp.zeros((4 * chans, LANES), jnp.bfloat16)
        parts_of = [zero if k is None else ref[k * 3 + place] for k in (early, late)]
        return jnp.concatenate(parts_of, axis=1)

    def pair_product(ref, base, used, start, count, weight_ref, taps_at):
        total = None
        for f in used:
            early, late = taps_at(f)
            for place in range(3):
                part = jnp.dot(
                    window(ref, place, base + f, start, count),
                    matrix(weight_ref, early, late, place),
                    preferred_element_type=jnp.float32,
                )
                total = part if total is None else total + part
        return total

    def inside(k):
        return k if 0 <= k <= 2 else None

    def ahead(f):
        return inside(f), inside(f - 1)

    def behind(f):
        return inside(2 - f), inside(3 - f)

    locals_in[0].wait()
    locals_in[1].wait()
    loop(2, put_act)
    loop(local, lambda f: put_act(2 + me * local + f))
    locals_in[2].wait()
    loop(local, lambda f: put_cot(me * local + f))
    locals_in[3].wait()

    def put_cache(frame):
        joined = jnp.concatenate(
            [mid_cache[frame, :, l * LANES : (l + 1) * LANES] for l in range(own)], axis=0
        )
        middle_t[frame] = jnp.transpose(joined)

    loop(2, put_cache)

    def strip(target, at, pieces):
        none = jnp.zeros((chans, chans), jnp.bfloat16)
        for place in range(4):
            left = pieces[place] if place < 3 else none
            right = pieces[place - 1] if place > 0 else none
            target[at, place * chans : (place + 1) * chans] = jnp.concatenate(
                [left, right], axis=1
            )

    def put_strips(index):
        strip(first_ref, index, [first_weight_ref[index * 3 + kq] for kq in range(3)])
        flipped = (index // 3 * 3 + 2 - lax.rem(index, 3)) * 3 + 2
        for target, source in (
            (second_back_ref, second_weight_ref),
            (first_back_ref, first_weight_ref),
        ):
            strip(target, index, [jnp.transpose(source[flipped - kq]) for kq in range(3)])

    locals_in[4].wait()
    locals_in[5].wait()
    locals_in[6].wait()
    loop(9, put_strips)

    for step, copy in enumerate(x_copies):
        copy.wait_recv()
        there = lax.rem(me + parts - step - 1, parts)
        loop(local, lambda f: put_act(2 + there * local + f))

    bias = bias_ref[...].reshape(1, chans)
    bias = jnp.concatenate([bias] * (LANES // chans), axis=1)

    def forward(pair):
        base = 2 * pair
        total = pair_product(act_taps, base, range(4), 0, held, first_ref, ahead)
        for u in range(2):
            pre = total[:, u * LANES : (u + 1) * LANES] + bias
            logistic = logistic_of(pre)
            slope[base + u] = logistic * (1.0 + pre * (1.0 - logistic))
            middle[base + u] = (pre * logistic).astype(jnp.bfloat16).reshape(held, height, LANES)
            mine = middle[base + u, pl.ds(offset, own)].reshape(own * height, LANES)
            middle_t[2 + base + u] = jnp.transpose(mine)

    loop(frames // 2, forward)

    def second_part(block, fresh):
        def at(place):
            total = None
            for f in range(local):
                frame = block * local + f
                left = middle_t[pl.ds(frame, 3)].reshape(3 * LANES, own * height)
                part = jnp.dot(
                    left,
                    window(cot_taps, place, frame, offset, own),
                    preferred_element_type=jnp.float32,
                )
                total = part if total is None else total + part
            second_acc[place] = total if fresh else second_acc[place] + total

        loop(3, at)

    def middle_part(block):
        for pair in range(local // 2):
            c = block * (local // 2) + pair
            for base, used, at in ((2 * c - 2, range(2, 4), c), (2 * c, range(2), c + 1)):
                middle_grad[at] += pair_product(
                    cot_taps, base, used, 0, held, second_back_ref, behind
                )

    middle_grad[...] = jnp.zeros_like(middle_grad)
    middle_part(me)
    second_part(me, True)
    for step, copy in enumerate(cot_copies):
        copy.wait_recv()
        there = lax.rem(me + parts - step - 1, parts)
        loop(local, lambda f: put_cot(there * local + f))
        second_part(there, False)

    half_lane = lax.broadcasted_iota(jnp.int32, (chans // 2, LANES), 1)

    def put_sum(which, index, value):
        value = value[:chans] + pltpu.roll(value[chans:], 3 * chans, 1)
        value = value * factor
        low, high = value[:, :LANES], value[:, LANES:]
        half = chans // 2
        tail = jnp.where(half_lane < chans, high[:half], pltpu.roll(high[half:], chans, 1))
        rows = jnp.concatenate([low, tail], axis=0)
        for n in range(3 * chans // 2 // ROWS):
            tile = index * (3 * chans // 2 // ROWS) + n
            tile = tile + (half_tiles - filled) * (tile // filled)
            sums[which, tile] = rows[n * ROWS : (n + 1) * ROWS]

    def put_second(place):
        value = second_acc[place]
        for kt in range(3):
            put_sum(0, kt * 3 + place, value[kt * LANES : (kt + 1) * LANES])

    mine = core * half_tiles
    other = (1 - core) * half_tiles
    whole = mine + rank * piece
    core_copies, ring, across, spread, last = [], [], [], [], []

    def swap_cores(which):
        for h in range(2):
            for n in range(filled, half_tiles):
                sums[which, h * half_tiles + n] = jnp.zeros((ROWS, LANES), jnp.float32)
        core_copies.append(
            pltpu.make_async_remote_copy(
                src_ref=sums.at[which, pl.ds(other, half_tiles)],
                dst_ref=sums_in.at[which],
                send_sem=core_send.at[0, which],
                recv_sem=core_recv.at[0, which],
                device_id=core_peer,
                device_id_type=MESH,
            )
        )
        core_copies[-1].start()

    def scatter(which):
        core_copies[which].wait_recv()

        def chip_sum(index):
            total = sums[which, mine + index] + sums_in[which, index]
            wire_own[which, index] = total
            wire[which, index] = total.astype(jnp.bfloat16)

        loop(half_tiles, chip_sum)
        copies = []
        for step in range(1, group):
            there, device = peer(step)
            copies.append(
                pltpu.make_async_remote_copy(
                    src_ref=wire.at[which, pl.ds(there * piece, piece)],
                    dst_ref=wire_in.at[which, step - 1],
                    send_sem=ring_send.at[0, which, step - 1],
                    recv_sem=ring_recv.at[0, which, step - 1],
                    device_id=device,
                    device_id_type=MESH,
                )
            )
        for copy in copies:
            copy.start()
        ring.append(copies)

    def reduce(which):
        for copy in ring[which]:
            copy.wait_recv()

        def slice_sum(index):
            total = wire_own[which, rank * piece + index]
            for step in range(1, group):
                total = total + wire_in[which, step - 1, index].astype(jnp.float32)
            piece_out[which, index] = total.astype(jnp.bfloat16)

        loop(piece, slice_sum)
        copies = []
        if not merged:
            for step in range(1, parts):
                copies.append(
                    pltpu.make_async_remote_copy(
                        src_ref=piece_out.at[which],
                        dst_ref=piece_in.at[which, me],
                        send_sem=part_send.at[which, step - 1],
                        recv_sem=part_recv.at[which, step - 1],
                        device_id={"tm": partner(step)},
                        device_id_type=MESH,
                    )
                )
                copies[-1].start()
            piece_in[which, me] = piece_out[which]
        across.append(copies)

    def publish(which):
        for copy in across[which]:
            copy.wait_recv()
        if merged:
            gathered[which, pl.ds(whole, piece)] = piece_out[which]
        else:

            def part_sum(index):
                total = piece_in[which, 0, index].astype(jnp.float32)
                for p in range(1, parts):
                    total = total + piece_in[which, p, index].astype(jnp.float32)
                gathered[which, whole + index] = total.astype(jnp.bfloat16)

            loop(piece, part_sum)
        copies = []
        for step in range(1, group):
            copies.append(
                pltpu.make_async_remote_copy(
                    src_ref=gathered.at[which, pl.ds(whole, piece)],
                    dst_ref=gathered.at[which, pl.ds(whole, piece)],
                    send_sem=ring_send.at[1, which, step - 1],
                    recv_sem=ring_recv.at[1, which, step - 1],
                    device_id=peer(step)[1],
                    device_id_type=MESH,
                )
            )
            copies[-1].start()
        spread.append(copies)

    def share(which):
        for copy in spread[which]:
            copy.wait_recv()
        last.append(
            pltpu.make_async_remote_copy(
                src_ref=gathered.at[which, pl.ds(mine, half_tiles)],
                dst_ref=gathered.at[which, pl.ds(mine, half_tiles)],
                send_sem=core_send.at[1, which],
                recv_sem=core_recv.at[1, which],
                device_id=core_peer,
                device_id_type=MESH,
            )
        )
        last[-1].start()

    loop(3, put_second)
    swap_cores(0)

    def lay_out(target, frame, u):
        for l in range(own):
            target[frame, :, l * LANES : (l + 1) * LANES] = staged[u, offset + l].astype(
                target.dtype
            )

    for step in range(1, parts):
        middle_part(lax.rem(me + parts - step, parts))
    first_pair = middle_grad[0]
    for u in range(2):
        staged[u] = first_pair[:, u * LANES : (u + 1) * LANES].reshape(held, height, LANES)
    for u in range(2):
        lay_out(mid_cache_out, u, u)

    def send_out(slot, source_of, target):
        copies = []
        for step in range(1, parts):
            there = partner(step)
            copies.append(
                pltpu.make_async_remote_copy(
                    src_ref=source_of(there),
                    dst_ref=target,
                    send_sem=out_send.at[slot, step - 1],
                    recv_sem=out_recv.at[slot, step - 1],
                    device_id={"tm": there},
                    device_id_type=MESH,
                )
            )
            copies[-1].start()
        outgoing.extend(copies)

    own_lanes = pl.ds(own_lane, own * LANES)

    def band_rows(index):
        return pl.ds(pl.multiple_of(index * band, ROWS), band)

    def send_cache(slot, source, target):
        if plan["direct"]:
            send_out(
                slot,
                lambda there: source.at[:, band_rows(there), :],
                target.at[0, :, :, own_lanes],
            )
            target[0, :, :, own_lanes] = source[:, band_rows(me), :]
        else:
            target[0] = source[...]

    outgoing = []
    scatter(0)
    send_cache(0, mid_cache_out, mid_cache_grad_ref)

    def put_pre(total, base):
        for u in range(2):
            grad = total[:, u * LANES : (u + 1) * LANES] * slope[base + u]
            put_taps(pre_taps, base + u, grad)
            at = frames + base + u
            middle[at] = grad.astype(jnp.bfloat16).reshape(held, height, LANES)
            mine = middle[at, pl.ds(offset, own)].reshape(own * height, LANES)
            pre_t[base + u] = jnp.transpose(mine)

    def inner_pair(pair):
        put_pre(middle_grad[pair + 1], 2 * pair)

    loop(frames // 2, inner_pair)

    def first_at(place):
        totals = [None] * 3
        for m in range(frames + 2):
            t0, t1 = max(0, m - 2), min(frames - 1, m)
            count = t1 - t0 + 1
            part = jnp.dot(
                pre_t[t0 : t1 + 1].reshape(count * LANES, own * height),
                window(act_taps, place, m, offset, own),
                preferred_element_type=jnp.float32,
            )
            for t in range(t0, t1 + 1):
                piece_of = part[(t - t0) * LANES : (t - t0 + 1) * LANES]
                kt = m - t
                totals[kt] = piece_of if totals[kt] is None else totals[kt] + piece_of
        for kt in range(3):
            put_sum(1, kt * 3 + place, totals[kt])

    loop(3, first_at)
    swap_cores(1)

    def put_ext(total, base, cached):
        for u in range(2):
            for l in range(own):
                lane = pl.multiple_of((offset + l) * LANES, LANES)
                value = ext[base + u, :, pl.ds(lane, LANES)].astype(jnp.float32)
                grad = (
                    total[l * height : (l + 1) * height, u * LANES : (u + 1) * LANES]
                    * slope_of(value)
                )
                place = slice(l * LANES, (l + 1) * LANES)
                if cached:
                    x_cache_out[base + u, :, place] = grad.astype(jnp.bfloat16)
                else:
                    given = cot[base + u - 2, :, pl.ds(lane, LANES)].astype(jnp.float32)
                    grad_out[base + u - 2, :, place] = (given + grad).astype(jnp.bfloat16)

    put_ext(
        pair_product(pre_taps, -2, range(2, 4), offset, own, first_back_ref, behind), 0, True
    )
    scatter(1)

    def send_grad(f):
        send_out(
            2 + f,
            lambda there: grad_out.at[there * local + f],
            grad_ref.at[0, f, :, own_lanes],
        )
        grad_ref[0, f, :, own_lanes] = grad_out[me * local + f]

    def inner_ext(pair):
        base = 2 * pair
        put_ext(
            pair_product(pre_taps, base - 2, range(4), offset, own, first_back_ref, behind),
            base,
            False,
        )

    send_cache(1, x_cache_out, x_cache_grad_ref)
    for pair in range(1, frames // 2):
        inner_ext(pair)
    reduce(0)
    put_ext(
        pair_product(pre_taps, frames - 2, range(2), offset, own, first_back_ref, behind),
        frames,
        False,
    )
    send_grad(0)
    publish(0)
    reduce(1)
    for f in range(1, local):
        send_grad(f)
    publish(1)
    share(0)
    last[0].wait_recv()

    def unpack(index):
        kt, place = index // 3, lax.rem(index, 3)
        for kq, value in enumerate(unpacked(plan, gathered, 0, index)):
            second_grad_ref[(kt * 3 + 2 - place) * 3 + 2 - kq] = value

    loop(9, unpack)
    share(1)
    last[1].wait_recv()
    gathered_ref[...] = gathered[1:2]

    for copy in outgoing:
        copy.wait()
    for copy in x_copies + cot_copies + core_copies + last:
        copy.wait_send()
    for copies in ring + spread + across:
        for copy in copies:
            copy.wait_send()


def unpacked(plan, ref, which, index):
    chans, filled = plan["chans"], plan["taps"] // 2
    skip = plan["group"] * plan["piece"] - filled
    tiles = []
    for n in range(3 * chans // 2 // ROWS):
        tile = index * (3 * chans // 2 // ROWS) + n
        tiles.append(ref[which, tile + skip * (tile // filled)])
    rows = jnp.concatenate(tiles, axis=0).astype(jnp.float32)
    tail = jnp.concatenate([rows[chans:, :chans], rows[chans:, chans:]], axis=0)
    return rows[:chans, :chans], rows[:chans, chans:], tail


def finish(plan, *refs):
    sources, gathered, targets = refs[:4], refs[4], refs[5:10]
    first, sems = refs[10:]
    leaving = [
        pltpu.make_async_copy(source, target, sems.at[n])
        for n, (source, target) in enumerate(zip(sources + (first,), targets))
    ]
    for copy in leaving[:4]:
        copy.start()

    def step(index, carry):
        for kq, value in enumerate(unpacked(plan, gathered, 0, index)):
            first[index * 3 + kq] = jnp.transpose(value)
        return carry

    lax.fori_loop(0, 9, step, 0)
    leaving[4].start()
    for copy in leaving:
        copy.wait()


def body(sizes, *arrays):
    (
        block_input,
        input_cache,
        middle_cache,
        first_weight,
        first_bias,
        second_weight,
        cotangent,
    ) = arrays
    plan = plan_of(sizes, block_input, first_weight)
    if not plan["fits"]:
        return plain_body(*arrays)
    chans, parts, local, frames = plan["chans"], plan["parts"], plan["local"], plan["frames"]
    height, own, held, rest = plan["height"], plan["own"], plan["held"], plan["rest"]
    piece, band, total = plan["piece"], plan["band"], plan["total"]
    count = block_input.shape[0] * plan["clips"] * frames * height * total * LANES // chans
    factor = 1.0 / math.sqrt(count)
    wide, mine = held * LANES, own * LANES
    group = plan["group"]
    tiles = group * piece
    bf16, f32 = jnp.bfloat16, jnp.float32
    if plan["direct"]:
        cache_shape = (1, 2, band, total * LANES)
    else:
        cache_shape = (1, 2, height, mine)
    hbm_spec = pl.BlockSpec(memory_space=pltpu.HBM)
    vmem_spec = pl.BlockSpec(memory_space=pltpu.VMEM)
    dma = pltpu.SemaphoreType.DMA
    weight_shape = jax.ShapeDtypeStruct((27, chans, chans), f32)
    outs = pl.pallas_call(
        functools.partial(kernel, plan, factor),
        out_shape=(
            jax.ShapeDtypeStruct(block_input.shape, bf16),
            jax.ShapeDtypeStruct(cache_shape, bf16),
            jax.ShapeDtypeStruct(cache_shape, bf16),
            weight_shape,
            jax.ShapeDtypeStruct((1, 2 * tiles, ROWS, LANES), bf16),
        ),
        in_specs=[hbm_spec] * 7,
        out_specs=(vmem_spec,) * 5,
        scratch_shapes=[
            pltpu.VMEM((frames + 2, height, wide), bf16),
            pltpu.VMEM((frames, height, wide), bf16),
            pltpu.VMEM((2, height, mine), bf16),
            pltpu.VMEM((3, frames + 2, held + 1, height, LANES), bf16),
            pltpu.VMEM((3, frames, held + 1, height, LANES), bf16),
            pltpu.VMEM((3, frames, held + 1, height, LANES), bf16),
            pltpu.VMEM((frames, held * height, LANES), f32),
            pltpu.VMEM((2 * frames, held, height, LANES), bf16),
            pltpu.VMEM((frames + 2, LANES, own * height), bf16),
            pltpu.VMEM((frames, LANES, own * height), bf16),
            pltpu.VMEM((2, held, height, LANES), f32),
            pltpu.VMEM((frames, height, mine), bf16),
            pltpu.VMEM((2, height, mine), bf16),
            pltpu.VMEM((2, height, mine), bf16),
            pltpu.VMEM((2, 2 * tiles, ROWS, LANES), f32),
            pltpu.VMEM((2, tiles, ROWS, LANES), f32),
            pltpu.VMEM((2, tiles, ROWS, LANES), f32),
            pltpu.VMEM((2, tiles, ROWS, LANES), bf16),
            pltpu.VMEM((2, group - 1, piece, ROWS, LANES), bf16),
            pltpu.VMEM((2, piece, ROWS, LANES), bf16),
            pltpu.VMEM((2, parts, piece, ROWS, LANES), bf16),
            pltpu.VMEM((2, 2 * tiles, ROWS, LANES), bf16),
            pltpu.VMEM((9, 4 * chans, LANES), bf16),
            pltpu.VMEM((9, 4 * chans, LANES), bf16),
            pltpu.VMEM((9, 4 * chans, LANES), bf16),
            pltpu.VMEM((3, 3 * LANES, 4 * chans), f32),
            pltpu.VMEM((frames // 2 + 1, held * height, 4 * chans), f32),
            pltpu.VMEM((27, chans, chans), bf16),
            pltpu.VMEM((27, chans, chans), bf16),
            pltpu.VMEM((chans,), f32),
            dma((7,)),
            dma((2, parts - 1)),
            dma((2, parts - 1)),
            dma((2 + local, parts - 1)),
            dma((2 + local, parts - 1)),
            dma((2, 2)),
            dma((2, 2)),
            dma((2, 2, group - 1)),
            dma((2, 2, group - 1)),
            dma((2, parts - 1)),
            dma((2, parts - 1)),
        ],
        compiler_params=pltpu.CompilerParams(
            collective_id=0, has_side_effects=True, vmem_limit_bytes=36 * 1024 * 1024
        ),
        name="block_backward",
    )(
        *(
            pltpu.with_memory_space_constraint(a, pltpu.HBM)
            for a in (
                block_input,
                input_cache,
                middle_cache,
                cotangent,
                first_weight.reshape(27, chans, chans),
                second_weight.reshape(27, chans, chans),
                first_bias,
            )
        )
    )
    results = outs[:4]
    outs = pl.pallas_call(
        functools.partial(finish, plan),
        out_shape=tuple(jax.ShapeDtypeStruct(a.shape, a.dtype) for a in results)
        + (weight_shape,),
        in_specs=[vmem_spec] * 5,
        out_specs=(hbm_spec,) * 5,
        scratch_shapes=[pltpu.VMEM(weight_shape.shape, f32), dma((5,))],
        compiler_params=pltpu.CompilerParams(vmem_limit_bytes=8 * 1024 * 1024),
        name="finish",
    )(*outs)
    grad, x_cache_grad, mid_cache_grad, second_grad, first_grad = outs
    if not plan["direct"]:
        x_cache_grad, mid_cache_grad = (
            lax.all_to_all(a, "tm", split_axis=2, concat_axis=3, tiled=True)
            for a in (x_cache_grad, mid_cache_grad)
        )
    shape = first_weight.shape
    return (
        grad,
        x_cache_grad,
        mid_cache_grad,
        first_grad.reshape(shape),
        second_grad.reshape(shape),
    )


def solution(mesh):
    return jax.shard_map(
        functools.partial(body, dict(mesh.shape)),
        mesh=mesh,
        in_specs=(
            P("clip", "tm", None, None),
            P("clip", None, None, None),
            P("clip", None, None, None),
            P(),
            P(),
            P(),
            P("clip", "tm", None, None),
        ),
        out_specs=(
            P("clip", "tm", None, None),
            P("clip", None, "tm", None),
            P("clip", None, "tm", None),
            P(),
            P(),
        ),
        check_vma=False,
    )
```

```python
import functools
import math

import jax
import jax.numpy as jnp
from jax import lax
from jax.experimental import pallas as pl
from jax.experimental.pallas import tpu as pltpu
from jax.sharding import PartitionSpec as P


def group_of(chans, width):
    group = max(1, 128 // chans)
    return group if width % group == 0 else 1


def bands_with_halo(array, axis, halo):
    count = lax.axis_size(axis)
    band = array.shape[2] // count
    padded = jnp.pad(array, ((0, 0), (0, 0), (halo, halo), (0, 0)))
    pieces = [
        lax.slice_in_dim(padded, p * band, p * band + band + 2 * halo, axis=2)
        for p in range(count)
    ]
    return lax.all_to_all(
        jnp.concatenate(pieces, axis=2), axis, split_axis=2, concat_axis=1, tiled=True
    )


def grouped(array, lanes):
    return array.reshape(array.shape[:-1] + (array.shape[-1] // lanes, lanes))


def patches(array, chans):
    zero = ((0, 0), (0, 0), (0, 0))
    before = jnp.pad(array[:, :, :, :-1, -chans:], zero + ((1, 0), (0, 0)))
    after = jnp.pad(array[:, :, :, 1:, :chans], zero + ((0, 1), (0, 0)))
    window = jnp.concatenate([before, array, after], axis=-1)
    rows = array.shape[2] - 2
    return jnp.concatenate([window[:, :, k : k + rows] for k in range(3)], axis=-1)


def matrix_of(weight, group):
    taps = jnp.transpose(weight, (1, 2, 3, 0, 4))
    zero = (0, 0)
    placed = jnp.stack(
        [jnp.pad(taps, (zero, (p, group - 1 - p), zero, zero, zero)) for p in range(group)],
        axis=4,
    )
    return placed.reshape(
        placed.shape[0] * placed.shape[1] * placed.shape[2], -1
    )


def product(source, matrix):
    return lax.dot_general(
        source, matrix, (((source.ndim - 1,), (0,)), ((), ())), preferred_element_type=jnp.float32
    )


def correlate(left, right):
    axes = tuple(range(left.ndim - 1))
    return lax.dot_general(
        left, right, ((axes, axes), ((), ())), preferred_element_type=jnp.float32
    )


def taps_of(block, group, first, second):
    block = block.reshape(3, group + 2, first, 3, group, second)
    total = None
    for p in range(group):
        part = block[:, p : p + 3, :, :, p, :]
        total = part if total is None else total + part
    return total


def silu_slope(value):
    logistic = jax.nn.sigmoid(value)
    return logistic * (1.0 + value * (1.0 - logistic))


def plain_body(
    block_input, input_cache, middle_cache, first_weight, first_bias, second_weight, cotangent
):
    chans = first_weight.shape[3]
    width = block_input.shape[3] // chans
    group = group_of(chans, width)
    lanes = group * chans
    height = block_input.shape[2]
    parts = lax.axis_size("tm")
    band = height // parts
    offset = lax.axis_index("tm") * band
    count = (
        block_input.shape[0] * lax.axis_size("clip") * block_input.shape[1] * parts * height * width
    )
    factor = 1.0 / math.sqrt(count)

    source = bands_with_halo(block_input, "tm", 2)
    upstream = grouped(bands_with_halo(cotangent, "tm", 2), lanes)
    padded_cache = jnp.pad(input_cache, ((0, 0), (0, 0), (2, 2), (0, 0)))
    cache_in = lax.dynamic_slice_in_dim(padded_cache, offset, band + 4, 2)
    cache_mid = grouped(lax.dynamic_slice_in_dim(middle_cache, offset, band, 2), lanes)
    extended = grouped(jnp.concatenate([cache_in, source], axis=1), lanes)
    frames = upstream.shape[1]

    activated = jax.nn.silu(extended.astype(jnp.float32)).astype(jnp.bfloat16)
    activated_patches = patches(activated, chans)
    forward = product(activated_patches, matrix_of(first_weight, group))
    pre = jnp.tile(first_bias, group)
    for kt in range(3):
        pre = pre + forward[:, kt : kt + frames, ..., kt * lanes : (kt + 1) * lanes]
    middle = jax.nn.silu(pre[:, :, 1:-1]).astype(jnp.bfloat16)
    middle_ext = jnp.concatenate([cache_mid, middle], axis=1)

    upstream_patches = patches(upstream, chans)
    middle_taps = jnp.concatenate(
        [middle_ext[:, kt : kt + frames] for kt in range(3)], axis=-1
    )
    second_block = correlate(upstream_patches[:, :, 1:-1], middle_taps)
    second_sum = taps_of(second_block, group, chans, chans) * factor
    second_sum = jnp.transpose(jnp.flip(second_sum, (0, 1)), (3, 0, 1, 4, 2))
    second_sum, upstream_patches = lax.optimization_barrier(
        (second_sum.reshape(-1, lanes), upstream_patches)
    )

    def input_grad_of(source_patches, weight):
        flipped = jnp.transpose(jnp.flip(weight, (1, 2)), (0, 1, 2, 4, 3))
        result = product(source_patches, matrix_of(flipped, group))
        total = None
        for kt in range(3):
            part = jnp.pad(
                result[..., kt * lanes : (kt + 1) * lanes],
                ((0, 0), (kt, 2 - kt), (0, 0), (0, 0), (0, 0)),
            )
            total = part if total is None else total + part
        return total

    middle_ext_grad = input_grad_of(upstream_patches, second_weight)
    row = offset - 1 + lax.broadcasted_iota(jnp.int32, (band + 2, 1, 1), 0)
    inside = (row >= 0) & (row < height)
    pre_grad = jnp.where(inside, middle_ext_grad[:, 2:] * silu_slope(pre), 0.0)
    pre_grad = pre_grad.astype(jnp.bfloat16)

    own_rows = pre_grad[:, :, 1:-1]
    grad_taps = jnp.concatenate(
        [
            jnp.pad(own_rows, ((0, 0), (kt, 2 - kt), (0, 0), (0, 0), (0, 0)))
            for kt in range(3)
        ],
        axis=-1,
    )
    first_block = correlate(activated_patches[:, :, 1:-1], grad_taps)
    first_sum = taps_of(first_block, group, chans, chans) * factor
    first_sum = jnp.transpose(first_sum, (3, 0, 1, 2, 4))
    first_sum, pre_grad = lax.optimization_barrier((first_sum.reshape(-1, lanes), pre_grad))
    first_total, second_total = lax.optimization_barrier(
        lax.psum((first_sum, second_sum), ("clip", "tm"))
    )

    activated_grad = input_grad_of(patches(pre_grad, chans), first_weight)
    own = extended[:, :, 2:-2].astype(jnp.float32)
    extended_grad = activated_grad * silu_slope(own)
    own_grad = upstream[:, :, 2:-2].astype(jnp.float32) + extended_grad[:, 2:]

    def merged(array):
        return array.astype(jnp.bfloat16).reshape(array.shape[:3] + (width * chans,))

    input_grad = lax.all_to_all(merged(own_grad), "tm", split_axis=1, concat_axis=2, tiled=True)
    return (
        input_grad,
        merged(extended_grad[:, :2]),
        merged(middle_ext_grad[:, :2, 1:-1]),
        first_total.reshape(first_weight.shape),
        second_total.reshape(second_weight.shape),
    )


LANES = 128
ROWS = 16
MESH = pl.DeviceIdType.MESH


def plan_of(sizes, block_input, first_weight):
    chans = first_weight.shape[3]
    parts, clips = sizes["tm"], sizes["clip"]
    local = block_input.shape[1]
    height = block_input.shape[2]
    total = block_input.shape[3] // LANES
    own = total // parts
    held = min(own + (1 if parts == 2 else 2), total)
    taps = 27 * chans // 2 // ROWS
    rest = clips // 2
    merged = rest * parts <= 8
    group = rest * parts if merged else rest
    piece = -(-(taps // 2) // group)
    fits = (
        2 * chans == LANES
        and height % 32 == 0
        and total % parts == 0
        and clips % 2 == 0
        and rest > 1
        and parts > 1
        and local % 2 == 0
        and taps % 2 == 0
    )
    return dict(
        fits=fits,
        chans=chans,
        parts=parts,
        clips=clips,
        local=local,
        frames=local * parts,
        height=height,
        total=total,
        own=own,
        held=held,
        taps=taps,
        rest=rest,
        merged=merged,
        group=group,
        piece=piece,
        band=height // parts,
        direct=(height // parts) % ROWS == 0,
    )


def kernel(
    plan,
    factor,
    x_ref,
    x_cache_ref,
    mid_cache_ref,
    cot_ref,
    first_hbm_ref,
    second_hbm_ref,
    bias_hbm_ref,
    grad_ref,
    x_cache_grad_ref,
    mid_cache_grad_ref,
    second_grad_ref,
    gathered_ref,
    ext,
    cot,
    mid_cache,
    act_taps,
    cot_taps,
    pre_taps,
    slope,
    middle,
    middle_t,
    pre_t,
    staged,
    grad_out,
    x_cache_out,
    mid_cache_out,
    sums,
    sums_in,
    wire_own,
    wire,
    wire_in,
    piece_out,
    piece_in,
    gathered,
    first_ref,
    second_back_ref,
    first_back_ref,
    second_acc,
    middle_grad,
    first_weight_ref,
    second_weight_ref,
    bias_ref,
    local_sem,
    ex_send,
    ex_recv,
    out_send,
    out_recv,
    core_send,
    core_recv,
    ring_send,
    ring_recv,
    part_send,
    part_recv,
):
    chans, parts, local, frames = plan["chans"], plan["parts"], plan["local"], plan["frames"]
    height, own, held, rest = plan["height"], plan["own"], plan["held"], plan["rest"]
    group, merged = plan["group"], plan["merged"]
    piece, band, taps = plan["piece"], plan["band"], plan["taps"]
    half_tiles = group * piece
    filled = taps // 2
    width = held * LANES
    me = lax.axis_index("tm")
    clip = lax.axis_index("clip")
    core = lax.rem(clip, 2)
    chip = clip // 2

    def first_group(index):
        return jnp.minimum(jnp.maximum(index * own - 1, 0), plan["total"] - held)

    def partner(step):
        return lax.rem(me + step, parts)

    rank = me * rest + chip if merged else chip

    def peer(step):
        there = lax.rem(rank + step, group)
        if merged:
            return there, {"clip": lax.rem(there, rest) * 2 + core, "tm": there // rest}
        return there, {"clip": there * 2 + core}

    core_peer = {"clip": clip + 1 - 2 * core}

    begin = first_group(me)
    offset = me * own - begin
    lane0 = pl.multiple_of(begin * LANES, LANES)
    own_lane = pl.multiple_of(me * own * LANES, LANES)

    locals_in = [
        pltpu.make_async_copy(
            x_ref.at[0, :, :, pl.ds(lane0, width)],
            ext.at[pl.ds(2 + me * local, local)],
            local_sem.at[0],
        ),
        pltpu.make_async_copy(
            x_cache_ref.at[0, :, :, pl.ds(lane0, width)], ext.at[pl.ds(0, 2)], local_sem.at[1]
        ),
        pltpu.make_async_copy(
            cot_ref.at[0, :, :, pl.ds(lane0, width)],
            cot.at[pl.ds(me * local, local)],
            local_sem.at[2],
        ),
        pltpu.make_async_copy(
            mid_cache_ref.at[0, :, :, pl.ds(own_lane, own * LANES)], mid_cache, local_sem.at[3]
        ),
    ]
    locals_in += [
        pltpu.make_async_copy(first_hbm_ref, first_weight_ref, local_sem.at[4]),
        pltpu.make_async_copy(second_hbm_ref, second_weight_ref, local_sem.at[5]),
        pltpu.make_async_copy(bias_hbm_ref, bias_ref, local_sem.at[6]),
    ]
    for copy in locals_in:
        copy.start()

    barrier = pltpu.get_barrier_semaphore()
    greeted = [core_peer] + [peer(step)[1] for step in range(1, group)]
    if not merged:
        greeted += [{"tm": partner(step)} for step in range(1, parts)]
    for there in greeted:
        pl.semaphore_signal(barrier, inc=1, device_id=there, device_id_type=MESH)
    pl.semaphore_wait(barrier, len(greeted))

    def exchange(index, source, target, base):
        copies = []
        for step in range(1, parts):
            there = partner(step)
            lane = pl.multiple_of(first_group(there) * LANES, LANES)
            copies.append(
                pltpu.make_async_remote_copy(
                    src_ref=source.at[0, :, :, pl.ds(lane, width)],
                    dst_ref=target.at[pl.ds(base + me * local, local)],
                    send_sem=ex_send.at[index, step - 1],
                    recv_sem=ex_recv.at[index, step - 1],
                    device_id={"tm": there},
                    device_id_type=MESH,
                )
            )
        for copy in copies:
            copy.start()
        return copies

    x_copies = exchange(0, x_ref, ext, 2)
    cot_copies = exchange(1, cot_ref, cot, 0)

    lane_of = lax.broadcasted_iota(jnp.int32, ((held + 1) * height, LANES), 1)
    row_of = lax.rem(
        lax.broadcasted_iota(jnp.int32, ((held + 1) * height, LANES), 0), height
    )

    def put_taps(target, frame, value):
        turned = pltpu.roll(value, chans, 1)
        zero = jnp.zeros((height, LANES), jnp.float32)
        moved = jnp.where(
            lane_of < chans,
            jnp.concatenate([zero, turned], axis=0),
            jnp.concatenate([turned, zero], axis=0),
        )
        count = moved.shape[0]
        above = jnp.where(row_of == 0, 0.0, pltpu.roll(moved, 1, 0))
        below = jnp.where(row_of == height - 1, 0.0, pltpu.roll(moved, count - 1, 0))
        for place, part in enumerate((above, moved, below)):
            target[place, frame] = part.astype(jnp.bfloat16).reshape(held + 1, height, LANES)

    def tiles_of(ref, frame):
        return jnp.concatenate(
            [ref[frame, :, l * LANES : (l + 1) * LANES] for l in range(held)], axis=0
        ).astype(jnp.float32)

    def logistic_of(value):
        return 1.0 / (1.0 + jnp.exp(-value))

    def slope_of(value):
        logistic = logistic_of(value)
        return logistic * (1.0 + value * (1.0 - logistic))

    def put_act(frame):
        value = tiles_of(ext, frame)
        put_taps(act_taps, frame, value * logistic_of(value))

    def put_cot(frame):
        put_taps(cot_taps, frame, tiles_of(cot, frame))

    def loop(count, call):
        def step(index, carry):
            call(index)
            return carry

        lax.fori_loop(0, count, step, 0)

    def window(ref, place, frame, start, count):
        left = ref[place, frame, pl.ds(start, count)].reshape(count * height, LANES)
        right = ref[place, frame, pl.ds(start + 1, count)].reshape(count * height, LANES)
        return jnp.concatenate([left, right], axis=1)

    def matrix(ref, early, late, place):
        zero = jnp.zeros((4 * chans, LANES), jnp.bfloat16)
        parts_of = [zero if k is None else ref[k * 3 + place] for k in (early, late)]
        return jnp.concatenate(parts_of, axis=1)

    def pair_product(ref, base, used, start, count, weight_ref, taps_at):
        total = None
        for f in used:
            early, late = taps_at(f)
            for place in range(3):
                part = jnp.dot(
                    window(ref, place, base + f, start, count),
                    matrix(weight_ref, early, late, place),
                    preferred_element_type=jnp.float32,
                )
                total = part if total is None else total + part
        return total

    def inside(k):
        return k if 0 <= k <= 2 else None

    def ahead(f):
        return inside(f), inside(f - 1)

    def behind(f):
        return inside(2 - f), inside(3 - f)

    locals_in[0].wait()
    locals_in[1].wait()
    loop(2, put_act)
    loop(local, lambda f: put_act(2 + me * local + f))
    locals_in[2].wait()
    loop(local, lambda f: put_cot(me * local + f))
    locals_in[3].wait()

    def put_cache(frame):
        joined = jnp.concatenate(
            [mid_cache[frame, :, l * LANES : (l + 1) * LANES] for l in range(own)], axis=0
        )
        middle_t[frame] = jnp.transpose(joined)

    loop(2, put_cache)

    def strip(target, at, pieces):
        none = jnp.zeros((chans, chans), jnp.bfloat16)
        for place in range(4):
            left = pieces[place] if place < 3 else none
            right = pieces[place - 1] if place > 0 else none
            target[at, place * chans : (place + 1) * chans] = jnp.concatenate(
                [left, right], axis=1
            )

    def put_strips(index):
        strip(first_ref, index, [first_weight_ref[index * 3 + kq] for kq in range(3)])
        flipped = (index // 3 * 3 + 2 - lax.rem(index, 3)) * 3 + 2
        for target, source in (
            (second_back_ref, second_weight_ref),
            (first_back_ref, first_weight_ref),
        ):
            strip(target, index, [jnp.transpose(source[flipped - kq]) for kq in range(3)])

    locals_in[4].wait()
    locals_in[5].wait()
    locals_in[6].wait()
    loop(9, put_strips)

    for step, copy in enumerate(x_copies):
        copy.wait_recv()
        there = lax.rem(me + parts - step - 1, parts)
        loop(local, lambda f: put_act(2 + there * local + f))

    bias = bias_ref[...].reshape(1, chans)
    bias = jnp.concatenate([bias] * (LANES // chans), axis=1)

    def forward(pair):
        base = 2 * pair
        total = pair_product(act_taps, base, range(4), 0, held, first_ref, ahead)
        for u in range(2):
            pre = total[:, u * LANES : (u + 1) * LANES] + bias
            logistic = logistic_of(pre)
            slope[base + u] = logistic * (1.0 + pre * (1.0 - logistic))
            middle[base + u] = (pre * logistic).astype(jnp.bfloat16).reshape(held, height, LANES)
            mine = middle[base + u, pl.ds(offset, own)].reshape(own * height, LANES)
            middle_t[2 + base + u] = jnp.transpose(mine)

    loop(frames // 2, forward)

    def second_part(block, fresh):
        def at(place):
            total = None
            for f in range(local):
                frame = block * local + f
                left = middle_t[pl.ds(frame, 3)].reshape(3 * LANES, own * height)
                part = jnp.dot(
                    left,
                    window(cot_taps, place, frame, offset, own),
                    preferred_element_type=jnp.float32,
                )
                total = part if total is None else total + part
            second_acc[place] = total if fresh else second_acc[place] + total

        loop(3, at)

    def middle_part(block):
        for pair in range(local // 2):
            c = block * (local // 2) + pair
            for base, used, at in ((2 * c - 2, range(2, 4), c), (2 * c, range(2), c + 1)):
                middle_grad[at] += pair_product(
                    cot_taps, base, used, 0, held, second_back_ref, behind
                )

    middle_grad[...] = jnp.zeros_like(middle_grad)
    middle_part(me)
    second_part(me, True)
    for step, copy in enumerate(cot_copies):
        copy.wait_recv()
        there = lax.rem(me + parts - step - 1, parts)
        loop(local, lambda f: put_cot(there * local + f))
        second_part(there, False)

    half_lane = lax.broadcasted_iota(jnp.int32, (chans // 2, LANES), 1)

    def put_sum(which, index, value):
        value = value[:chans] + pltpu.roll(value[chans:], 3 * chans, 1)
        value = value * factor
        low, high = value[:, :LANES], value[:, LANES:]
        half = chans // 2
        tail = jnp.where(half_lane < chans, high[:half], pltpu.roll(high[half:], chans, 1))
        rows = jnp.concatenate([low, tail], axis=0)
        for n in range(3 * chans // 2 // ROWS):
            tile = index * (3 * chans // 2 // ROWS) + n
            tile = tile + (half_tiles - filled) * (tile // filled)
            sums[which, tile] = rows[n * ROWS : (n + 1) * ROWS]

    def put_second(place):
        value = second_acc[place]
        for kt in range(3):
            put_sum(0, kt * 3 + place, value[kt * LANES : (kt + 1) * LANES])

    mine = core * half_tiles
    other = (1 - core) * half_tiles
    whole = mine + rank * piece
    core_copies, ring, across, spread, last = [], [], [], [], []

    def swap_cores(which):
        for h in range(2):
            for n in range(filled, half_tiles):
                sums[which, h * half_tiles + n] = jnp.zeros((ROWS, LANES), jnp.float32)
        core_copies.append(
            pltpu.make_async_remote_copy(
                src_ref=sums.at[which, pl.ds(other, half_tiles)],
                dst_ref=sums_in.at[which],
                send_sem=core_send.at[0, which],
                recv_sem=core_recv.at[0, which],
                device_id=core_peer,
                device_id_type=MESH,
            )
        )
        core_copies[-1].start()

    def scatter(which):
        core_copies[which].wait_recv()

        def chip_sum(index):
            total = sums[which, mine + index] + sums_in[which, index]
            wire_own[which, index] = total
            wire[which, index] = total.astype(jnp.bfloat16)

        loop(half_tiles, chip_sum)
        copies = []
        for step in range(1, group):
            there, device = peer(step)
            copies.append(
                pltpu.make_async_remote_copy(
                    src_ref=wire.at[which, pl.ds(there * piece, piece)],
                    dst_ref=wire_in.at[which, step - 1],
                    send_sem=ring_send.at[0, which, step - 1],
                    recv_sem=ring_recv.at[0, which, step - 1],
                    device_id=device,
                    device_id_type=MESH,
                )
            )
        for copy in copies:
            copy.start()
        ring.append(copies)

    def reduce(which):
        for copy in ring[which]:
            copy.wait_recv()

        def slice_sum(index):
            total = wire_own[which, rank * piece + index]
            for step in range(1, group):
                total = total + wire_in[which, step - 1, index].astype(jnp.float32)
            piece_out[which, index] = total.astype(jnp.bfloat16)

        loop(piece, slice_sum)
        copies = []
        if not merged:
            for step in range(1, parts):
                copies.append(
                    pltpu.make_async_remote_copy(
                        src_ref=piece_out.at[which],
                        dst_ref=piece_in.at[which, me],
                        send_sem=part_send.at[which, step - 1],
                        recv_sem=part_recv.at[which, step - 1],
                        device_id={"tm": partner(step)},
                        device_id_type=MESH,
                    )
                )
                copies[-1].start()
            piece_in[which, me] = piece_out[which]
        across.append(copies)

    def publish(which):
        for copy in across[which]:
            copy.wait_recv()
        if merged:
            gathered[which, pl.ds(whole, piece)] = piece_out[which]
        else:

            def part_sum(index):
                total = piece_in[which, 0, index].astype(jnp.float32)
                for p in range(1, parts):
                    total = total + piece_in[which, p, index].astype(jnp.float32)
                gathered[which, whole + index] = total.astype(jnp.bfloat16)

            loop(piece, part_sum)
        copies = []
        for step in range(1, group):
            copies.append(
                pltpu.make_async_remote_copy(
                    src_ref=gathered.at[which, pl.ds(whole, piece)],
                    dst_ref=gathered.at[which, pl.ds(whole, piece)],
                    send_sem=ring_send.at[1, which, step - 1],
                    recv_sem=ring_recv.at[1, which, step - 1],
                    device_id=peer(step)[1],
                    device_id_type=MESH,
                )
            )
            copies[-1].start()
        spread.append(copies)

    def share(which):
        for copy in spread[which]:
            copy.wait_recv()
        last.append(
            pltpu.make_async_remote_copy(
                src_ref=gathered.at[which, pl.ds(mine, half_tiles)],
                dst_ref=gathered.at[which, pl.ds(mine, half_tiles)],
                send_sem=core_send.at[1, which],
                recv_sem=core_recv.at[1, which],
                device_id=core_peer,
                device_id_type=MESH,
            )
        )
        last[-1].start()

    loop(3, put_second)
    swap_cores(0)

    def lay_out(target, frame, u):
        for l in range(own):
            target[frame, :, l * LANES : (l + 1) * LANES] = staged[u, offset + l].astype(
                target.dtype
            )

    for step in range(1, parts):
        middle_part(lax.rem(me + parts - step, parts))
    first_pair = middle_grad[0]
    for u in range(2):
        staged[u] = first_pair[:, u * LANES : (u + 1) * LANES].reshape(held, height, LANES)
    for u in range(2):
        lay_out(mid_cache_out, u, u)

    def send_out(slot, source_of, target):
        copies = []
        for step in range(1, parts):
            there = partner(step)
            copies.append(
                pltpu.make_async_remote_copy(
                    src_ref=source_of(there),
                    dst_ref=target,
                    send_sem=out_send.at[slot, step - 1],
                    recv_sem=out_recv.at[slot, step - 1],
                    device_id={"tm": there},
                    device_id_type=MESH,
                )
            )
            copies[-1].start()
        outgoing.extend(copies)

    own_lanes = pl.ds(own_lane, own * LANES)

    def band_rows(index):
        return pl.ds(pl.multiple_of(index * band, ROWS), band)

    def send_cache(slot, source, target):
        if plan["direct"]:
            send_out(
                slot,
                lambda there: source.at[:, band_rows(there), :],
                target.at[0, :, :, own_lanes],
            )
            target[0, :, :, own_lanes] = source[:, band_rows(me), :]
        else:
            target[0] = source[...]

    outgoing = []
    scatter(0)
    send_cache(0, mid_cache_out, mid_cache_grad_ref)

    def put_pre(total, base):
        for u in range(2):
            grad = total[:, u * LANES : (u + 1) * LANES] * slope[base + u]
            put_taps(pre_taps, base + u, grad)
            at = frames + base + u
            middle[at] = grad.astype(jnp.bfloat16).reshape(held, height, LANES)
            mine = middle[at, pl.ds(offset, own)].reshape(own * height, LANES)
            pre_t[base + u] = jnp.transpose(mine)

    def inner_pair(pair):
        put_pre(middle_grad[pair + 1], 2 * pair)

    loop(frames // 2, inner_pair)

    def first_at(place):
        totals = [None] * 3
        for m in range(frames + 2):
            t0, t1 = max(0, m - 2), min(frames - 1, m)
            count = t1 - t0 + 1
            part = jnp.dot(
                pre_t[t0 : t1 + 1].reshape(count * LANES, own * height),
                window(act_taps, place, m, offset, own),
                preferred_element_type=jnp.float32,
            )
            for t in range(t0, t1 + 1):
                piece_of = part[(t - t0) * LANES : (t - t0 + 1) * LANES]
                kt = m - t
                totals[kt] = piece_of if totals[kt] is None else totals[kt] + piece_of
        for kt in range(3):
            put_sum(1, kt * 3 + place, totals[kt])

    loop(3, first_at)
    swap_cores(1)

    def put_ext(total, base, cached):
        for u in range(2):
            for l in range(own):
                lane = pl.multiple_of((offset + l) * LANES, LANES)
                value = ext[base + u, :, pl.ds(lane, LANES)].astype(jnp.float32)
                grad = (
                    total[l * height : (l + 1) * height, u * LANES : (u + 1) * LANES]
                    * slope_of(value)
                )
                place = slice(l * LANES, (l + 1) * LANES)
                if cached:
                    x_cache_out[base + u, :, place] = grad.astype(jnp.bfloat16)
                else:
                    given = cot[base + u - 2, :, pl.ds(lane, LANES)].astype(jnp.float32)
                    grad_out[base + u - 2, :, place] = (given + grad).astype(jnp.bfloat16)

    put_ext(
        pair_product(pre_taps, -2, range(2, 4), offset, own, first_back_ref, behind), 0, True
    )
    scatter(1)

    def send_grad(f):
        send_out(
            2 + f,
            lambda there: grad_out.at[there * local + f],
            grad_ref.at[0, f, :, own_lanes],
        )
        grad_ref[0, f, :, own_lanes] = grad_out[me * local + f]

    def inner_ext(pair):
        base = 2 * pair
        put_ext(
            pair_product(pre_taps, base - 2, range(4), offset, own, first_back_ref, behind),
            base,
            False,
        )

    send_cache(1, x_cache_out, x_cache_grad_ref)
    for pair in range(1, frames // 2):
        inner_ext(pair)
    reduce(0)
    put_ext(
        pair_product(pre_taps, frames - 2, range(2), offset, own, first_back_ref, behind),
        frames,
        False,
    )
    send_grad(0)
    publish(0)
    reduce(1)
    for f in range(1, local):
        send_grad(f)
    publish(1)
    share(0)
    last[0].wait_recv()

    def unpack(index):
        kt, place = index // 3, lax.rem(index, 3)
        for kq, value in enumerate(unpacked(plan, gathered, 0, index)):
            second_grad_ref[(kt * 3 + 2 - place) * 3 + 2 - kq] = value

    loop(9, unpack)
    share(1)
    last[1].wait_recv()
    gathered_ref[...] = gathered[1:2]

    for copy in outgoing:
        copy.wait()
    for copy in x_copies + cot_copies + core_copies + last:
        copy.wait_send()
    for copies in ring + spread + across:
        for copy in copies:
            copy.wait_send()


def unpacked(plan, ref, which, index):
    chans, filled = plan["chans"], plan["taps"] // 2
    skip = plan["group"] * plan["piece"] - filled
    tiles = []
    for n in range(3 * chans // 2 // ROWS):
        tile = index * (3 * chans // 2 // ROWS) + n
        tiles.append(ref[which, tile + skip * (tile // filled)])
    rows = jnp.concatenate(tiles, axis=0).astype(jnp.float32)
    tail = jnp.concatenate([rows[chans:, :chans], rows[chans:, chans:]], axis=0)
    return rows[:chans, :chans], rows[:chans, chans:], tail


def finish(plan, *refs):
    sources, gathered, targets = refs[:4], refs[4], refs[5:10]
    first, sems = refs[10:]
    leaving = [
        pltpu.make_async_copy(source, target, sems.at[n])
        for n, (source, target) in enumerate(zip(sources, targets))
    ]
    for copy in leaving:
        copy.start()
    for kt in range(3):

        def step(index, carry):
            for kq, value in enumerate(unpacked(plan, gathered, 0, index)):
                first[index * 3 + kq] = jnp.transpose(value)
            return carry

        lax.fori_loop(3 * kt, 3 * kt + 3, step, 0)
        rows = pl.ds(9 * kt, 9)
        leaving.append(
            pltpu.make_async_copy(first.at[rows], targets[4].at[rows], sems.at[4 + kt])
        )
        leaving[-1].start()
    for copy in leaving:
        copy.wait()


def body(sizes, *arrays):
    (
        block_input,
        input_cache,
        middle_cache,
        first_weight,
        first_bias,
        second_weight,
        cotangent,
    ) = arrays
    plan = plan_of(sizes, block_input, first_weight)
    if not plan["fits"]:
        return plain_body(*arrays)
    chans, parts, local, frames = plan["chans"], plan["parts"], plan["local"], plan["frames"]
    height, own, held, rest = plan["height"], plan["own"], plan["held"], plan["rest"]
    piece, band, total = plan["piece"], plan["band"], plan["total"]
    count = block_input.shape[0] * plan["clips"] * frames * height * total * LANES // chans
    factor = 1.0 / math.sqrt(count)
    wide, mine = held * LANES, own * LANES
    group = plan["group"]
    tiles = group * piece
    bf16, f32 = jnp.bfloat16, jnp.float32
    if plan["direct"]:
        cache_shape = (1, 2, band, total * LANES)
    else:
        cache_shape = (1, 2, height, mine)
    hbm_spec = pl.BlockSpec(memory_space=pltpu.HBM)
    vmem_spec = pl.BlockSpec(memory_space=pltpu.VMEM)
    dma = pltpu.SemaphoreType.DMA
    weight_shape = jax.ShapeDtypeStruct((27, chans, chans), f32)
    outs = pl.pallas_call(
        functools.partial(kernel, plan, factor),
        out_shape=(
            jax.ShapeDtypeStruct(block_input.shape, bf16),
            jax.ShapeDtypeStruct(cache_shape, bf16),
            jax.ShapeDtypeStruct(cache_shape, bf16),
            weight_shape,
            jax.ShapeDtypeStruct((1, 2 * tiles, ROWS, LANES), bf16),
        ),
        in_specs=[hbm_spec] * 7,
        out_specs=(vmem_spec,) * 5,
        scratch_shapes=[
            pltpu.VMEM((frames + 2, height, wide), bf16),
            pltpu.VMEM((frames, height, wide), bf16),
            pltpu.VMEM((2, height, mine), bf16),
            pltpu.VMEM((3, frames + 2, held + 1, height, LANES), bf16),
            pltpu.VMEM((3, frames, held + 1, height, LANES), bf16),
            pltpu.VMEM((3, frames, held + 1, height, LANES), bf16),
            pltpu.VMEM((frames, held * height, LANES), f32),
            pltpu.VMEM((2 * frames, held, height, LANES), bf16),
            pltpu.VMEM((frames + 2, LANES, own * height), bf16),
            pltpu.VMEM((frames, LANES, own * height), bf16),
            pltpu.VMEM((2, held, height, LANES), f32),
            pltpu.VMEM((frames, height, mine), bf16),
            pltpu.VMEM((2, height, mine), bf16),
            pltpu.VMEM((2, height, mine), bf16),
            pltpu.VMEM((2, 2 * tiles, ROWS, LANES), f32),
            pltpu.VMEM((2, tiles, ROWS, LANES), f32),
            pltpu.VMEM((2, tiles, ROWS, LANES), f32),
            pltpu.VMEM((2, tiles, ROWS, LANES), bf16),
            pltpu.VMEM((2, group - 1, piece, ROWS, LANES), bf16),
            pltpu.VMEM((2, piece, ROWS, LANES), bf16),
            pltpu.VMEM((2, parts, piece, ROWS, LANES), bf16),
            pltpu.VMEM((2, 2 * tiles, ROWS, LANES), bf16),
            pltpu.VMEM((9, 4 * chans, LANES), bf16),
            pltpu.VMEM((9, 4 * chans, LANES), bf16),
            pltpu.VMEM((9, 4 * chans, LANES), bf16),
            pltpu.VMEM((3, 3 * LANES, 4 * chans), f32),
            pltpu.VMEM((frames // 2 + 1, held * height, 4 * chans), f32),
            pltpu.VMEM((27, chans, chans), bf16),
            pltpu.VMEM((27, chans, chans), bf16),
            pltpu.VMEM((chans,), f32),
            dma((7,)),
            dma((2, parts - 1)),
            dma((2, parts - 1)),
            dma((2 + local, parts - 1)),
            dma((2 + local, parts - 1)),
            dma((2, 2)),
            dma((2, 2)),
            dma((2, 2, group - 1)),
            dma((2, 2, group - 1)),
            dma((2, parts - 1)),
            dma((2, parts - 1)),
        ],
        compiler_params=pltpu.CompilerParams(
            collective_id=0, has_side_effects=True, vmem_limit_bytes=36 * 1024 * 1024
        ),
        name="block_backward",
    )(
        *(
            pltpu.with_memory_space_constraint(a, pltpu.HBM)
            for a in (
                block_input,
                input_cache,
                middle_cache,
                cotangent,
                first_weight.reshape(27, chans, chans),
                second_weight.reshape(27, chans, chans),
                first_bias,
            )
        )
    )
    results = outs[:4]
    outs = pl.pallas_call(
        functools.partial(finish, plan),
        out_shape=tuple(jax.ShapeDtypeStruct(a.shape, a.dtype) for a in results)
        + (weight_shape,),
        in_specs=[vmem_spec] * 5,
        out_specs=(hbm_spec,) * 5,
        scratch_shapes=[pltpu.VMEM(weight_shape.shape, f32), dma((7,))],
        compiler_params=pltpu.CompilerParams(vmem_limit_bytes=8 * 1024 * 1024),
        name="finish",
    )(*outs)
    grad, x_cache_grad, mid_cache_grad, second_grad, first_grad = outs
    if not plan["direct"]:
        x_cache_grad, mid_cache_grad = (
            lax.all_to_all(a, "tm", split_axis=2, concat_axis=3, tiled=True)
            for a in (x_cache_grad, mid_cache_grad)
        )
    shape = first_weight.shape
    return (
        grad,
        x_cache_grad,
        mid_cache_grad,
        first_grad.reshape(shape),
        second_grad.reshape(shape),
    )


def solution(mesh):
    return jax.shard_map(
        functools.partial(body, dict(mesh.shape)),
        mesh=mesh,
        in_specs=(
            P("clip", "tm", None, None),
            P("clip", None, None, None),
            P("clip", None, None, None),
            P(),
            P(),
            P(),
            P("clip", "tm", None, None),
        ),
        out_specs=(
            P("clip", "tm", None, None),
            P("clip", None, "tm", None),
            P("clip", None, "tm", None),
            P(),
            P(),
        ),
        check_vma=False,
    )
```
